128 devices in a mesh: det: 4 (over x), tm: 32 (over z, y, core).
Axes of the slice: x: 4, y: 4, z: 4, core: 2. Of those that a mesh axis runs over, the one named last changes fastest.
Arguments:
- sol_map: float32 [3, 196608], P(None, ('det', 'tm')), may hold values from -6 to 6
- resid_map: float32 [3, 196608], P(None, ('det', 'tm')), may hold values from -6 to 6
- direction: float32 [3, 196608], P(None, ('det', 'tm')), may hold values from -6 to 6
- precond: float32 [3, 196608], P(None, ('det', 'tm')), may hold values from 0.1 to 1
- pixels: int32 [128, 65536], P('det', 'tm'), may hold values from 0 to 196607
- angle_index: int32 [128, 65536], P('det', 'tm'), may hold values from 0 to 127
- angles: float32 [128], replicated, may hold values from -3.140625 to 3.140625
- flag_mask: int32 [128, 65536], P('det', 'tm'), may hold values 0 or 1
- inv_noise: float32 [128, 32769], P(('det', 'tm')), may hold values from 0.05 to 1
Outputs:
- new_sol: float32 [3, 196608], P(None, ('det', 'tm'))
- new_resid: float32 [3, 196608], P(None, ('det', 'tm'))
- new_dir: float32 [3, 196608], P(None, ('det', 'tm'))
- new_norm: float32 [], replicated
The draws below stay inside these ranges and needn't reach their ends.
All inputs are finite; a program needn't handle non-finite values. No bound on the sum of `flag_mask` on one device may be relied on, other than what follows from the above.
Results may differ from the reference program's by a relative error of at most 0.0001.
Values sent between devices are 32-bit elements; how exact they have to be, the bound alone decides.
No kernel may reach another device: no remote copies, remote signals or barrier semaphores. Data moves between devices by JAX's collectives and lax.ppermute only.
A program may use at most 320 MiB of HBM per device.

```python
import math
import jax
import jax.numpy as jnp
from jax import lax

NSAMP = 65536
NDET = 128
NPIX = 196608
NANG = 128
NFREQ = 32769


def touch_ends(values, own_key, smallest, largest):
    shape = values.shape
    index_at = [jax.random.randint(jax.random.fold_in(own_key, axis), (), 0, shape[axis]) for axis in range(len(shape))]
    values = values.at[tuple(index_at)].set(smallest)
    longest = shape.index(max(shape))
    index_at[longest] = (index_at[longest] + 1) % shape[longest]
    return values.at[tuple(index_at)].set(largest)


def block_scale(key, dims, cuts, smallest, largest):
    def one(dim, parts):
        heights = jax.random.uniform(jax.random.fold_in(jax.random.fold_in(key, 6), dim), (parts,), jnp.float32, smallest / len(cuts), largest / len(cuts))
        return jnp.repeat(jnp.exp(heights), dims[dim] // parts).reshape((-1,) + (1,) * (len(dims) - dim - 1))

    loudness = one(*cuts[0])
    for cut in cuts[1:]:
        loudness = loudness * one(*cut)
    return loudness


def bell_draw(rng, dims, spread, limit, split=(), kind=jnp.bfloat16):
    values = jax.random.normal(rng, dims, jnp.float32) * spread
    if len(split) > 0:
        values = block_scale(rng, dims, split, -0.22, 0.18) * values
    return jnp.clip(values, min=-limit, max=limit).astype(kind)


def setup_inputs(seed: int = 0) -> dict:
    key_of = jax.random.split(jax.random.key(seed), 10)
    return {
        "sol_map": bell_draw(key_of[0], (3, NPIX), 1.0, 6.0, ((1, 128),), jnp.float32),
        "resid_map": bell_draw(key_of[1], (3, NPIX), 1.0, 6.0, ((1, 128),), jnp.float32),
        "direction": bell_draw(key_of[2], (3, NPIX), 1.0, 6.0, ((1, 128),), jnp.float32),
        "precond": jnp.clip(jnp.exp(math.log(1.0) - 2.3025851 * jax.random.uniform(key_of[3], (3, NPIX), jnp.float32) ** block_scale(key_of[3], (3, NPIX), ((1, 128),), -0.2, 0.2)), 0.1, 1.0),
        "pixels": touch_ends(jax.random.randint(key_of[4], (NDET, NSAMP), 0, NPIX), jax.random.fold_in(key_of[4], 1), 0, NPIX - 1).astype(jnp.int32),
        "angle_index": touch_ends(jax.random.randint(key_of[5], (NDET, NSAMP), 0, NANG), jax.random.fold_in(key_of[5], 1), 0, NANG - 1).astype(jnp.int32),
        "angles": jnp.clip(jax.random.uniform(key_of[6], (NANG,), jnp.float32, -3.140625, 3.140625), -3.140625, 3.140625),
        "flag_mask": touch_ends((jax.random.randint(key_of[7], (NDET, NSAMP), 0, 16) < 15).astype(jnp.int32), jax.random.fold_in(key_of[7], 1), 0, 1),
        "inv_noise": jnp.clip(jnp.exp(math.log(1.0) - 2.9957323 * jax.random.uniform(key_of[8], (NDET, NFREQ), jnp.float32) ** block_scale(key_of[8], (NDET, NFREQ), ((0, 128),), -0.2, 0.2)), 0.05, 1.0),
    }


def reference(sol_map, resid_map, direction, precond, pixels, angle_index, angles, flag_mask, inv_noise):
    cos_table = jnp.cos(2.0 * angles)
    sin_table = jnp.sin(2.0 * angles)
    row_block = 64

    def one_block(image, block_id):
        head_row = block_id * row_block
        pix_rows = lax.dynamic_slice_in_dim(pixels, head_row, row_block, 0)
        ang_rows = lax.dynamic_slice_in_dim(angle_index, head_row, row_block, 0)
        usable = lax.dynamic_slice_in_dim(flag_mask, head_row, row_block, 0).astype(jnp.float32)
        filt_rows = lax.dynamic_slice_in_dim(inv_noise, head_row, row_block, 0)
        cos_two = cos_table[ang_rows]
        sin_two = sin_table[ang_rows]
        signal = usable * (direction[0][pix_rows] + direction[1][pix_rows] * cos_two + direction[2][pix_rows] * sin_two)
        spectrum = jnp.fft.rfft(signal, axis=1)
        filtered = jnp.fft.irfft(spectrum * filt_rows, n=NSAMP, axis=1).astype(jnp.float32)
        weighted = usable * filtered
        contrib = jnp.stack([weighted, weighted * cos_two, weighted * sin_two]).reshape(3, -1)
        image = image.at[:, pix_rows.reshape(-1)].add(contrib)
        return image, None

    image, _ = lax.scan(one_block, jnp.zeros((3, NPIX), jnp.float32), jnp.arange(NDET // row_block, dtype=jnp.int32))
    norm_old = jnp.sum(resid_map * precond * resid_map)
    curvature = jnp.sum(direction * image)
    step_size = norm_old / curvature
    new_sol = sol_map + step_size * direction
    new_resid = resid_map - step_size * image
    new_norm = jnp.sum(new_resid * precond * new_resid)
    new_dir = precond * new_resid + (new_norm / norm_old) * direction
    return new_sol, new_resid, new_dir, new_norm
```

```python
import functools
import math

import jax
import jax.numpy as jnp
import numpy as np
from jax import lax
from jax.experimental import pallas as pl
from jax.experimental.pallas import tpu as pltpu
from jax.sharding import Mesh
from jax.sharding import PartitionSpec as P

DET_TM = ("det", "tm_0", "tm_1", "tm_2")
TM = ("tm_0", "tm_1", "tm_2")
CHIPS = ("det", "tm_0", "tm_1")
CORE = "tm_2"

LANES = 128
CHUNK = 256
WINDOW = 16
UNROLL = 32
VMEM = pl.BlockSpec(memory_space=pltpu.VMEM)
SMEM = pl.BlockSpec(memory_space=pltpu.SMEM)


def exchange(array, axes):
    return lax.all_to_all(array, axes, split_axis=0, concat_axis=0, tiled=True)


def halves(values):
    high = values.astype(jnp.bfloat16)
    return high, (values - high.astype(jnp.float32)).astype(jnp.bfloat16)


def dot(left, right, dims=(((1,), (0,)), ((), ()))):
    return lax.dot_general(left, right, dims, preferred_element_type=jnp.float32)


def dot3(left, right):
    return dot(left[0], right[0]) + (dot(left[0], right[1]) + dot(left[1], right[0]))


def weights_kernel(payload_ref, trig_ref, out_ref):
    cos_row = jnp.broadcast_to(trig_ref[0:1, :], (8, LANES))
    sin_row = jnp.broadcast_to(trig_ref[1:2, :], (8, LANES))

    def step(block, carry):
        for part in range(4):
            row = pl.multiple_of(block * 32, 32) + 8 * part
            payload = payload_ref[pl.ds(row, 8), :]
            angle = (payload >> 16) & (LANES - 1)
            usable = (payload >> 23).astype(jnp.float32)
            out_ref[0, pl.ds(row, 8), :] = usable
            out_ref[1, pl.ds(row, 8), :] = usable * jnp.take_along_axis(cos_row, angle, axis=1, mode="promise_in_bounds")
            out_ref[2, pl.ds(row, 8), :] = usable * jnp.take_along_axis(sin_row, angle, axis=1, mode="promise_in_bounds")
        return carry

    lax.fori_loop(0, payload_ref.shape[0] // 32, step, 0)


def pair(tile, chunk):
    return jnp.concatenate([tile[2 * chunk : 2 * chunk + 1], tile[2 * chunk + 1 : 2 * chunk + 2]], axis=1)


def one_hot_low(pixel_row):
    low = (pixel_row & (LANES - 1)).astype(jnp.float32).astype(jnp.bfloat16)
    level = lax.broadcasted_iota(jnp.int32, (LANES, CHUNK), 0).astype(jnp.float32).astype(jnp.bfloat16)
    return jnp.where(jnp.broadcast_to(low, level.shape) == level, jnp.bfloat16(1.0), jnp.bfloat16(0.0))


def window_mask(pixel_row, base):
    level = lax.broadcasted_iota(jnp.int32, (WINDOW, CHUNK), 0)
    return ((pixel_row >> 7) - base) == level


def gather_window(tab_ref, pixel_row, weight_rows, base):
    pieces = []
    for comp in range(3):
        pieces.extend(halves(tab_ref[comp, pl.ds(base, WINDOW), :]))
    found = dot(jnp.concatenate(pieces, axis=0), one_hot_low(pixel_row))
    total = None
    for comp in range(3):
        lo = 2 * comp * WINDOW
        value = (found[lo : lo + WINDOW] + found[lo + WINDOW : lo + 2 * WINDOW]) * weight_rows[comp]
        total = value if total is None else total + value
    return jnp.sum(jnp.where(window_mask(pixel_row, base), total, 0.0), axis=0, keepdims=True)


def first_base(first_ref, chunk):
    return pl.multiple_of((first_ref[chunk] >> 10) << 3, 8)


def window_count(first_ref, last_ref, chunk):
    return (((last_ref[chunk] >> 7) - first_base(first_ref, chunk)) >> 4) + 1


def more_windows(first_ref, last_ref, step, one):
    counts = [window_count(first_ref, last_ref, step * UNROLL + u) for u in range(UNROLL)]

    @pl.when(functools.reduce(jnp.maximum, counts) > 1)
    def _():
        def each(u, carry):
            chunk = step * UNROLL + u
            base = first_base(first_ref, chunk)

            def more(w, inner):
                one(chunk, pl.multiple_of(base + w * WINDOW, 8))
                return inner

            return lax.fori_loop(1, window_count(first_ref, last_ref, chunk), more, carry)

        lax.fori_loop(0, UNROLL, each, 0)


def dyn_pair(ref, chunk, *lead):
    rows = [ref[(*lead, pl.ds(2 * chunk + h, 1), slice(None))] for h in range(2)]
    return jnp.concatenate(rows, axis=1)


def gather_kernel(first_ref, last_ref, pix_ref, weight_ref, full_ref, out_ref, tab_ref):
    share_rows = full_ref.shape[1] // 3

    def lay(couple, carry):
        row = pl.multiple_of(couple * 2 * share_rows, 8)
        for comp in range(3):
            parts = [full_ref[2 * couple + h, comp * share_rows : (comp + 1) * share_rows, :] for h in range(2)]
            tab_ref[comp, pl.ds(row, 2 * share_rows), :] = jnp.concatenate(parts, axis=0)
        return carry

    lax.fori_loop(0, full_ref.shape[0] // 2, lay, 0)
    map_rows = full_ref.shape[0] * share_rows
    tab_ref[:, map_rows:, :] = jnp.zeros((3, tab_ref.shape[1] - map_rows, LANES), jnp.float32)

    def step(it, carry):
        row = pl.multiple_of(it * 2 * UNROLL, 8)
        pix = pix_ref[pl.ds(row, 2 * UNROLL), :]
        weights = [weight_ref[comp, pl.ds(row, 2 * UNROLL), :] for comp in range(3)]
        rows = []
        for u in range(UNROLL):
            value = gather_window(tab_ref, pair(pix, u), [pair(w, u) for w in weights], first_base(first_ref, it * UNROLL + u))
            rows.extend([value[:, :LANES], value[:, LANES:]])
        out_ref[pl.ds(row, 2 * UNROLL), :] = jnp.concatenate(rows, axis=0)

        def one(chunk, base):
            value = gather_window(
                tab_ref, dyn_pair(pix_ref, chunk), [dyn_pair(weight_ref, chunk, comp) for comp in range(3)], base
            )
            for h in range(2):
                out_ref[pl.ds(2 * chunk + h, 1), :] += value[:, h * LANES : (h + 1) * LANES]

        more_windows(first_ref, last_ref, it, one)
        return carry

    lax.fori_loop(0, pix_ref.shape[0] // (2 * UNROLL), step, 0)


def scatter_window(pixel_row, value_rows, base):
    mask = window_mask(pixel_row, base)
    pieces = []
    for value in value_rows:
        high = value.astype(jnp.bfloat16).astype(jnp.float32)
        for part in (high, value - high):
            pieces.append(jnp.where(mask, part, 0.0).astype(jnp.bfloat16))
    sums = dot(jnp.concatenate(pieces, axis=0), one_hot_low(pixel_row), (((1,), (1,)), ((), ())))
    return [sums[2 * c * WINDOW : (2 * c + 1) * WINDOW] + sums[(2 * c + 1) * WINDOW : (2 * c + 2) * WINDOW] for c in range(3)]


def scatter_kernel(first_ref, last_ref, pix_ref, weight_ref, value_ref, out_ref, map_ref):
    map_ref[...] = jnp.zeros(map_ref.shape, jnp.float32)

    def add(sums, base):
        for comp in range(3):
            map_ref[comp, pl.ds(base, WINDOW), :] += sums[comp]

    def step(it, carry):
        row = pl.multiple_of(it * 2 * UNROLL, 8)
        pix = pix_ref[pl.ds(row, 2 * UNROLL), :]
        value = value_ref[pl.ds(row, 2 * UNROLL), :]
        contrib = [value * weight_ref[comp, pl.ds(row, 2 * UNROLL), :] for comp in range(3)]
        bases = [first_base(first_ref, it * UNROLL + u) for u in range(UNROLL)]
        sums = [scatter_window(pair(pix, u), [pair(c, u) for c in contrib], bases[u]) for u in range(UNROLL)]
        for u in range(UNROLL):
            add(sums[u], bases[u])

        def one(chunk, base):
            held = dyn_pair(value_ref, chunk)
            add(scatter_window(dyn_pair(pix_ref, chunk), [held * dyn_pair(weight_ref, chunk, c) for c in range(3)], base), base)

        more_windows(first_ref, last_ref, it, one)
        return carry

    lax.fori_loop(0, pix_ref.shape[0] // (2 * UNROLL), step, 0)
    share_rows = out_ref.shape[2] // 3

    def lay(chip, carry):
        row = pl.multiple_of(chip * 2 * share_rows, 8)
        for comp in range(3):
            both = map_ref[comp, pl.ds(row, 2 * share_rows), :]
            for core in range(2):
                out_ref[core, chip, comp * share_rows : (comp + 1) * share_rows, :] = both[core * share_rows : (core + 1) * share_rows]
        return carry

    lax.fori_loop(0, out_ref.shape[1], lay, 0)


def filter_tables(side):
    index = np.arange(side)
    turn = 2.0 * np.pi / side * ((index[:, None] * index[None, :]) % side)
    twist = 2.0 * np.pi / (side * side) * (index[:, None] * index[None, :])

    def split(values):
        high = values.astype(np.float32).astype(jnp.bfloat16)
        return high, (values - high.astype(np.float64)).astype(np.float32).astype(jnp.bfloat16)

    forms = np.stack([*split(np.cos(turn)), *split(-np.sin(turn))])
    twists = np.stack([np.cos(twist), -np.sin(twist)]).astype(np.float32)
    return forms, twists


def filter_kernel(form_ref, twist_ref, weight_ref, tail_ref, x_ref, out_ref):
    side = form_ref.shape[1]
    half = side // 2
    total = side * side
    f_real = (form_ref[0], form_ref[1])
    f_imag = (form_ref[2], form_ref[3])
    w_real, w_imag = twist_ref[0], twist_ref[1]
    x = jnp.concatenate([x_ref[pl.ds(0, side, 2), :], x_ref[pl.ds(1, side, 2), :]], axis=1)
    xs = halves(x)
    y_real = dot3(f_real, xs)
    y_imag = dot3(f_imag, xs)
    y_real, y_imag = halves(y_real * w_real - y_imag * w_imag), halves(y_real * w_imag + y_imag * w_real)
    left_real = (f_real[0][:, :half], f_real[1][:, :half])
    left_imag = (f_imag[0][:, :half], f_imag[1][:, :half])
    weight = weight_ref[...]
    z_real = halves((dot3(y_real, left_real) - dot3(y_imag, left_imag)) * weight)
    z_imag = halves((dot3(y_real, left_imag) + dot3(y_imag, left_real)) * weight)
    top_real = (f_real[0][:half], f_real[1][:half])
    top_imag = (f_imag[0][:half], f_imag[1][:half])
    v_real = dot3(z_real, top_real) + dot3(z_imag, top_imag)
    v_imag = dot3(z_imag, top_real) - dot3(z_real, top_imag)
    v_real, v_imag = halves(v_real * w_real + v_imag * w_imag), halves(v_imag * w_real - v_real * w_imag)
    result = dot3(f_real, v_real) + dot3(f_imag, v_imag)
    sign = jnp.where((lax.broadcasted_iota(jnp.int32, (1, side), 1) & 1) == 0, 1.0, -1.0)
    last = jnp.sum(jnp.sum(x, axis=0, keepdims=True) * sign, axis=1, keepdims=True) * tail_ref[0]
    result = (result + last * sign) * (1.0 / total)
    out_ref[pl.ds(0, side, 2), :] = result[:, :half]
    out_ref[pl.ds(1, side, 2), :] = result[:, half:]


def body(sol_map, resid_map, direction, precond, pixels, angle_index, angles, flag_mask, inv_noise, forms, twists):
    share_len = direction.shape[1]
    n_dev = lax.axis_size(DET_TM)
    n_pixels = share_len * n_dev
    map_rows = n_pixels // LANES
    share_rows = share_len // LANES
    det_rows, samples = pixels.shape
    total = det_rows * samples
    side = math.isqrt(total)
    rows = total // LANES
    f32 = jnp.float32

    pointing = jnp.stack([a.reshape(det_rows, samples // LANES, LANES) for a in (pixels, angle_index, flag_mask)], axis=1)
    pointing = exchange(pointing, TM)

    own = direction.reshape(1, 3 * share_rows, LANES)
    full = exchange(jnp.broadcast_to(own, (n_dev, 3 * share_rows, LANES)), DET_TM)

    time_ids = jnp.arange(total, dtype=jnp.int32)
    pix = pointing[:, 0].reshape(total)
    payload = time_ids + (pointing[:, 1].reshape(total) << 16) + (pointing[:, 2].reshape(total) << 23)
    pix, payload = lax.sort((pix, payload), num_keys=1, is_stable=False)
    order = payload & 0xFFFF
    rank = lax.sort((order, time_ids), num_keys=1, is_stable=False)[1]
    payload, rank = lax.optimization_barrier((payload, rank))
    order = payload & 0xFFFF
    by_chunk = pix.reshape(total // CHUNK, CHUNK)
    first, last = by_chunk[:, 0], by_chunk[:, CHUNK - 1]
    pix = pix.reshape(rows, LANES)
    trig = jnp.stack([jnp.cos(2.0 * angles), jnp.sin(2.0 * angles)])
    weights = pl.pallas_call(
        weights_kernel, in_specs=[VMEM, VMEM], out_specs=VMEM, out_shape=jax.ShapeDtypeStruct((3, rows, LANES), f32)
    )(payload.reshape(rows, LANES), trig)

    signal = pl.pallas_call(
        gather_kernel,
        in_specs=[SMEM, SMEM, VMEM, VMEM, VMEM],
        out_specs=VMEM,
        out_shape=jax.ShapeDtypeStruct((rows, LANES), f32),
        scratch_shapes=[pltpu.VMEM((3, map_rows + 8, LANES), f32)],
    )(first, last, pix, weights, full)
    signal = lax.sort((order, signal.reshape(total)), num_keys=1, is_stable=False)[1]

    doubled = inv_noise[0, : total // 2].reshape(side // 2, side).T * 2.0
    corner = jnp.zeros((side, side // 2), jnp.bool_).at[0, 0].set(True)
    doubled = jnp.where(corner, inv_noise[0, 0], doubled)
    filtered = pl.pallas_call(
        filter_kernel,
        in_specs=[VMEM, VMEM, VMEM, SMEM, VMEM],
        out_specs=VMEM,
        out_shape=jax.ShapeDtypeStruct((rows, LANES), f32),
    )(forms, twists, doubled, inv_noise[0, total // 2 :], signal.reshape(rows, LANES))
    filtered = lax.sort((rank, filtered.reshape(total)), num_keys=1, is_stable=False)[1]

    shares = pl.pallas_call(
        scatter_kernel,
        in_specs=[SMEM, SMEM, VMEM, VMEM, VMEM],
        out_specs=VMEM,
        out_shape=jax.ShapeDtypeStruct((2, n_dev // 2, 3 * share_rows, LANES), f32),
        scratch_shapes=[pltpu.VMEM((3, map_rows + 8, LANES), f32)],
    )(first, last, pix, weights, filtered.reshape(rows, LANES))

    shares = jnp.sum(exchange(shares, CORE), axis=0)
    image = jnp.sum(exchange(shares, CHIPS), axis=0).reshape(3, share_len)

    scaled_resid = precond * resid_map
    scalars = jnp.stack(
        [
            jnp.sum(scaled_resid * resid_map),
            jnp.sum(direction * image),
            jnp.sum(image * scaled_resid),
            jnp.sum(image * precond * image),
        ]
    )
    scalars = jnp.pad(scalars, (0, LANES - 4)).reshape(1, 1, LANES)
    scalars = jnp.sum(exchange(jnp.broadcast_to(scalars, (n_dev, 1, LANES)), DET_TM), axis=(0, 1))
    norm_old, curvature, cross_term, image_norm = scalars[0], scalars[1], scalars[2], scalars[3]
    step_size = norm_old / curvature
    new_resid = resid_map - step_size * image
    new_norm = norm_old - 2.0 * step_size * cross_term + step_size * step_size * image_norm
    new_sol = sol_map + step_size * direction
    new_dir = precond * new_resid + new_norm / norm_old * direction
    return (new_sol, new_resid, new_dir, new_norm)


def solution(mesh):
    split = Mesh(mesh.devices.reshape(mesh.shape["det"], 4, 4, 2), DET_TM)
    mapped = jax.shard_map(
        body,
        mesh=split,
        in_specs=(
            P(None, DET_TM),
            P(None, DET_TM),
            P(None, DET_TM),
            P(None, DET_TM),
            P("det", TM),
            P("det", TM),
            P(),
            P("det", TM),
            P(DET_TM, None),
            P(),
            P(),
        ),
        out_specs=(P(None, DET_TM), P(None, DET_TM), P(None, DET_TM), P()),
        check_vma=False,
    )

    def run(sol_map, resid_map, direction, precond, pixels, angle_index, angles, flag_mask, inv_noise):
        forms, twists = filter_tables(math.isqrt(pixels.shape[1]))
        return mapped(
            sol_map, resid_map, direction, precond, pixels, angle_index, angles, flag_mask, inv_noise, jnp.asarray(forms), jnp.asarray(twists)
        )

    return run
```

```python
import functools
import math

import jax
import jax.numpy as jnp
import numpy as np
from jax import lax
from jax.experimental import pallas as pl
from jax.experimental.pallas import tpu as pltpu
from jax.sharding import Mesh
from jax.sharding import PartitionSpec as P

DET_TM = ("det", "tm_0", "tm_1", "tm_2")
TM = ("tm_0", "tm_1", "tm_2")
CHIPS = ("det", "tm_0", "tm_1")
CORE = "tm_2"

LANES = 128
CHUNK = 256
WINDOW = 16
ROWS = 16
VMEM = pl.BlockSpec(memory_space=pltpu.VMEM)
SMEM = pl.BlockSpec(memory_space=pltpu.SMEM)


def exchange(array, axes):
    return lax.all_to_all(array, axes, split_axis=0, concat_axis=0, tiled=True)


def halves(values):
    high = values.astype(jnp.bfloat16)
    return high, (values - high.astype(jnp.float32)).astype(jnp.bfloat16)


def dot(left, right, dims=(((1,), (0,)), ((), ()))):
    return lax.dot_general(left, right, dims, preferred_element_type=jnp.float32)


def dot3(left, right):
    return dot(left[0], right[0]) + (dot(left[0], right[1]) + dot(left[1], right[0]))


LEVELS = 16
CHUNK_BITS = 8
TILES = 64
SLOTS = LEVELS * (LEVELS - 1) + 2 * LEVELS


def tile(ref, index):
    return ref.at[8 * index : 8 * index + 8, :]


def partner(values, bit):
    axis, size, step = (0, 8, 1 << (bit - 5)) if bit < 8 else (1, LANES, 1 << (bit - 9))
    if 2 * step == size:
        return pltpu.roll(values, step, axis)
    upper = (lax.broadcasted_iota(jnp.int32, (8, LANES), axis) & step) != 0
    return jnp.where(upper, pltpu.roll(values, step, axis), pltpu.roll(values, size - step, axis))


def tile_pairs(bit):
    step = 1 << (5 if bit == 8 else bit)
    return [(i, i + step) for i in range(TILES) if not i & step]


def is_tile_bit(bit):
    return bit < 5 or bit == 8


def word(position):
    return jnp.int32(-(1 << 31) if position == 31 else 1 << position)


def slot(level, bit):
    return level * (level - 1) + 2 * bit


def in_network(level, bit):
    return jnp.logical_and(bit < level, jnp.logical_or(level < LEVELS, bit >= CHUNK_BITS))


def place(tile_index):
    inside = lax.broadcasted_iota(jnp.int32, (8, LANES), 0) * 32 + lax.broadcasted_iota(jnp.int32, (8, LANES), 1) * 512
    return inside + ((tile_index & 31) + ((tile_index >> 5) << 8))


def sort_stage(key_ref, mask_ref, level, bit):
    at = slot(level, bit)
    if is_tile_bit(bit):
        bits = jnp.zeros((8, LANES), jnp.int32)
        for position, (low, high) in enumerate(tile_pairs(bit)):
            a, b = tile(key_ref, low)[...], tile(key_ref, high)[...]
            swap = a > b
            tile(key_ref, low)[...] = jnp.where(swap, b, a)
            tile(key_ref, high)[...] = jnp.where(swap, a, b)
            bits = bits | jnp.where(swap, word(position), 0)
        mask_ref[at] = bits
        return
    axis, step = (0, 1 << (bit - 5)) if bit < 8 else (1, 1 << (bit - 9))
    upper = -((lax.broadcasted_iota(jnp.int32, (8, LANES), axis) & step) // step)
    for part in range(2):
        bits = jnp.zeros((8, LANES), jnp.int32)
        for position in range(32):
            view = tile(key_ref, 32 * part + position)
            own = view[...]
            other = partner(own, bit)
            swap = (own ^ upper) > (other ^ upper)
            view[...] = jnp.where(swap, other, own)
            bits = bits | jnp.where(swap, word(position), 0)
        mask_ref[at + part] = bits


def replay_stage(data_ref, mask_ref, level, bit):
    at = slot(level, bit)
    if is_tile_bit(bit):
        bits = mask_ref[at]
        for position, (low, high) in enumerate(tile_pairs(bit)):
            a, b = tile(data_ref, low)[...], tile(data_ref, high)[...]
            swap = (bits & word(position)) != 0
            tile(data_ref, low)[...] = jnp.where(swap, b, a)
            tile(data_ref, high)[...] = jnp.where(swap, a, b)
        return
    for part in range(2):
        bits = mask_ref[at + part]
        for position in range(32):
            view = tile(data_ref, 32 * part + position)
            own = view[...]
            view[...] = jnp.where((bits & word(position)) != 0, partner(own, bit), own)


def network(stage, backwards=False, before=None):
    def one_level(count, carry):
        level = LEVELS - count if backwards else count + 1
        if before is not None:
            before(level)
        for bit in range(LEVELS) if backwards else reversed(range(LEVELS)):
            pl.when(in_network(level, bit))(functools.partial(stage, level, bit))
        return carry

    lax.fori_loop(0, LEVELS, one_level, 0)


def sort_kernel(pointing_ref, trig_ref, pix_ref, weight_ref, bound_ref, mask_ref, key_ref):
    blocks, _, block_rows, _ = pointing_ref.shape
    for block in range(blocks):
        packed = pointing_ref[block, 0] * 256 + pointing_ref[block, 1] * 2 + pointing_ref[block, 2]
        key_ref[block * block_rows : (block + 1) * block_rows, :] = packed
    for index in range(TILES):
        tile(key_ref, index)[...] ^= -(place(index) & 1)

    def turn(level):
        for index in range(TILES):
            at = place(index)
            tile(key_ref, index)[...] ^= -(((at >> level) ^ (at >> (level - 1))) & 1)

    network(functools.partial(sort_stage, key_ref, mask_ref), before=turn)

    half = key_ref.shape[0] // 2
    for h in range(2):
        keys = key_ref[h * half : (h + 1) * half, :]
        bound_ref[h : h + 1, :] = jnp.min(keys, axis=0, keepdims=True) >> 8
        bound_ref[2 + h : 3 + h, :] = jnp.max(keys, axis=0, keepdims=True) >> 8
    cos_row = jnp.broadcast_to(trig_ref[0:1, :], (8, LANES))
    sin_row = jnp.broadcast_to(trig_ref[1:2, :], (8, LANES))
    for part in range(4):
        keys = key_ref[part * LANES : (part + 1) * LANES, :].T
        cols = slice(part * LANES, (part + 1) * LANES)
        pix_ref[:, cols] = keys >> 8
        for row in range(0, LANES, 8):
            key = keys[row : row + 8]
            angle = (key >> 1) & (LANES - 1)
            usable = (key & 1).astype(jnp.float32)
            weight_ref[0, row : row + 8, cols] = usable
            weight_ref[1, row : row + 8, cols] = usable * jnp.take_along_axis(cos_row, angle, axis=1, mode="promise_in_bounds")
            weight_ref[2, row : row + 8, cols] = usable * jnp.take_along_axis(sin_row, angle, axis=1, mode="promise_in_bounds")


def one_hot_low(pixel_row):
    low = (pixel_row & (LANES - 1)).astype(jnp.float32).astype(jnp.bfloat16)
    level = lax.broadcasted_iota(jnp.int32, (LANES, CHUNK), 0).astype(jnp.float32).astype(jnp.bfloat16)
    return jnp.where(jnp.broadcast_to(low, level.shape) == level, jnp.bfloat16(1.0), jnp.bfloat16(0.0))


def window_mask(pixel_row, base):
    level = lax.broadcasted_iota(jnp.int32, (WINDOW, CHUNK), 0)
    return ((pixel_row >> 7) - base) == level


def gather_window(tab_ref, pixel_row, weight_rows, base):
    pieces = []
    for comp in range(3):
        pieces.extend(halves(tab_ref[comp, pl.ds(base, WINDOW), :]))
    found = dot(jnp.concatenate(pieces, axis=0), one_hot_low(pixel_row))
    total = None
    for comp in range(3):
        lo = 2 * comp * WINDOW
        value = (found[lo : lo + WINDOW] + found[lo + WINDOW : lo + 2 * WINDOW]) * weight_rows[comp]
        total = value if total is None else total + value
    return jnp.sum(jnp.where(window_mask(pixel_row, base), total, 0.0), axis=0, keepdims=True)


def first_base(bound_ref, row, half):
    return pl.multiple_of((bound_ref[half, row] >> 10) << 3, 8)


def window_count(bound_ref, row, half):
    return (((bound_ref[2 + half, row] >> 7) - first_base(bound_ref, row, half)) >> 4) + 1


def more_windows(bound_ref, head, one):
    counts = [window_count(bound_ref, head + r, h) for r in range(ROWS) for h in range(2)]

    @pl.when(functools.reduce(jnp.maximum, counts) > 1)
    def _():
        def each(r, carry):
            for h in range(2):
                base = first_base(bound_ref, head + r, h)

                def more(w, inner, h=h, base=base):
                    one(head + r, h, pl.multiple_of(base + w * WINDOW, 8))
                    return inner

                lax.fori_loop(1, window_count(bound_ref, head + r, h), more, 0)
            return carry

        lax.fori_loop(0, ROWS, each, 0)


def cut(values, r, h):
    return values[r : r + 1, h * CHUNK : (h + 1) * CHUNK]


def held(ref, row, h, *lead):
    return ref[(*lead, pl.ds(row, 1), slice(h * CHUNK, (h + 1) * CHUNK))]


def gather_all(bound_ref, pix_ref, weight_ref, tab_ref, out_ref):
    def step(it, carry):
        head = pl.multiple_of(it * ROWS, 8)
        pix = pix_ref[pl.ds(head, ROWS), :]
        weights = [weight_ref[comp, pl.ds(head, ROWS), :] for comp in range(3)]
        rows = []
        for r in range(ROWS):
            parts = [
                gather_window(tab_ref, cut(pix, r, h), [cut(w, r, h) for w in weights], first_base(bound_ref, head + r, h)) for h in range(2)
            ]
            rows.append(jnp.concatenate(parts, axis=1))
        out_ref[pl.ds(head, ROWS), :] = jnp.concatenate(rows, axis=0)

        def one(row, h, base):
            value = gather_window(tab_ref, held(pix_ref, row, h), [held(weight_ref, row, h, comp) for comp in range(3)], base)
            out_ref[pl.ds(row, 1), h * CHUNK : (h + 1) * CHUNK] += value

        more_windows(bound_ref, head, one)
        return carry

    lax.fori_loop(0, pix_ref.shape[0] // ROWS, step, 0)


def scatter_window(pixel_row, value_rows, base):
    mask = window_mask(pixel_row, base)
    pieces = []
    for value in value_rows:
        high = value.astype(jnp.bfloat16).astype(jnp.float32)
        for part in (high, value - high):
            pieces.append(jnp.where(mask, part, 0.0).astype(jnp.bfloat16))
    sums = dot(jnp.concatenate(pieces, axis=0), one_hot_low(pixel_row), (((1,), (1,)), ((), ())))
    return [sums[2 * c * WINDOW : (2 * c + 1) * WINDOW] + sums[(2 * c + 1) * WINDOW : (2 * c + 2) * WINDOW] for c in range(3)]


def scatter_all(bound_ref, pix_ref, weight_ref, value_ref, map_ref):
    map_ref[...] = jnp.zeros(map_ref.shape, jnp.float32)

    def add(sums, base):
        for comp in range(3):
            map_ref[comp, pl.ds(base, WINDOW), :] += sums[comp]

    def step(it, carry):
        head = pl.multiple_of(it * ROWS, 8)
        pix = pix_ref[pl.ds(head, ROWS), :]
        value = value_ref[pl.ds(head, ROWS), :]
        contrib = [value * weight_ref[comp, pl.ds(head, ROWS), :] for comp in range(3)]
        places = [(r, h) for r in range(ROWS) for h in range(2)]
        bases = [first_base(bound_ref, head + r, h) for r, h in places]
        sums = [scatter_window(cut(pix, r, h), [cut(c, r, h) for c in contrib], base) for (r, h), base in zip(places, bases)]
        for base, one_sum in zip(bases, sums):
            add(one_sum, base)

        def one(row, h, base):
            value = held(value_ref, row, h)
            add(scatter_window(held(pix_ref, row, h), [value * held(weight_ref, row, h, c) for c in range(3)], base), base)

        more_windows(bound_ref, head, one)
        return carry

    lax.fori_loop(0, pix_ref.shape[0] // ROWS, step, 0)


def main_kernel(
    bound_ref, tail_ref, pix_ref, weight_ref, mask_ref, full_ref, form_ref, twist_ref, filt_ref, out_ref, tab_ref, series_ref, wide_ref
):
    share_rows = full_ref.shape[1] // 3
    map_rows = full_ref.shape[0] * share_rows

    def lay(couple, carry):
        row = pl.multiple_of(couple * 2 * share_rows, 8)
        for comp in range(3):
            parts = [full_ref[2 * couple + h, comp * share_rows : (comp + 1) * share_rows, :] for h in range(2)]
            tab_ref[comp, pl.ds(row, 2 * share_rows), :] = jnp.concatenate(parts, axis=0)
        return carry

    lax.fori_loop(0, full_ref.shape[0] // 2, lay, 0)
    tab_ref[:, map_rows:, :] = jnp.zeros((3, tab_ref.shape[1] - map_rows, LANES), jnp.float32)

    gather_all(bound_ref, pix_ref, weight_ref, tab_ref, wide_ref)
    for part in range(4):
        series_ref[part * LANES : (part + 1) * LANES, :] = wide_ref[:, part * LANES : (part + 1) * LANES].T
    network(functools.partial(replay_stage, series_ref, mask_ref), backwards=True)
    filter_series(form_ref, twist_ref, filt_ref, tail_ref, series_ref)
    network(functools.partial(replay_stage, series_ref, mask_ref))
    for part in range(4):
        wide_ref[:, part * LANES : (part + 1) * LANES] = series_ref[part * LANES : (part + 1) * LANES, :].T
    scatter_all(bound_ref, pix_ref, weight_ref, wide_ref, tab_ref)

    def spread(chip, carry):
        row = pl.multiple_of(chip * 2 * share_rows, 8)
        for comp in range(3):
            both = tab_ref[comp, pl.ds(row, 2 * share_rows), :]
            for core in range(2):
                out_ref[core, chip, comp * share_rows : (comp + 1) * share_rows, :] = both[core * share_rows : (core + 1) * share_rows]
        return carry

    lax.fori_loop(0, out_ref.shape[1], spread, 0)


def filter_tables(side):
    index = np.arange(side)
    turn = 2.0 * np.pi / side * ((index[:, None] * index[None, :]) % side)
    twist = 2.0 * np.pi / (side * side) * (index[:, None] * index[None, :])

    def split(values):
        high = values.astype(np.float32).astype(jnp.bfloat16)
        return high, (values - high.astype(np.float64)).astype(np.float32).astype(jnp.bfloat16)

    forms = np.stack([*split(np.cos(turn)), *split(-np.sin(turn))])
    twists = np.stack([np.cos(twist), -np.sin(twist)]).astype(np.float32)
    return forms, twists


def filter_series(form_ref, twist_ref, weight_ref, tail_ref, x_ref):
    side = form_ref.shape[1]
    half = side // 2
    total = side * side
    f_real = (form_ref[0], form_ref[1])
    f_imag = (form_ref[2], form_ref[3])
    w_real, w_imag = twist_ref[0], twist_ref[1]
    x = jnp.concatenate([x_ref[pl.ds(0, side, 2), :], x_ref[pl.ds(1, side, 2), :]], axis=1)
    xs = halves(x)
    y_real = dot3(f_real, xs)
    y_imag = dot3(f_imag, xs)
    y_real, y_imag = halves(y_real * w_real - y_imag * w_imag), halves(y_real * w_imag + y_imag * w_real)
    left_real = (f_real[0][:, :half], f_real[1][:, :half])
    left_imag = (f_imag[0][:, :half], f_imag[1][:, :half])
    weight = weight_ref[...]
    z_real = halves((dot3(y_real, left_real) - dot3(y_imag, left_imag)) * weight)
    z_imag = halves((dot3(y_real, left_imag) + dot3(y_imag, left_real)) * weight)
    top_real = (f_real[0][:half], f_real[1][:half])
    top_imag = (f_imag[0][:half], f_imag[1][:half])
    v_real = dot3(z_real, top_real) + dot3(z_imag, top_imag)
    v_imag = dot3(z_imag, top_real) - dot3(z_real, top_imag)
    v_real, v_imag = halves(v_real * w_real + v_imag * w_imag), halves(v_imag * w_real - v_real * w_imag)
    result = dot3(f_real, v_real) + dot3(f_imag, v_imag)
    sign = jnp.where((lax.broadcasted_iota(jnp.int32, (1, side), 1) & 1) == 0, 1.0, -1.0)
    last = jnp.sum(jnp.sum(x, axis=0, keepdims=True) * sign, axis=1, keepdims=True) * tail_ref[0]
    result = (result + last * sign) * (1.0 / total)
    x_ref[pl.ds(0, side, 2), :] = result[:, :half]
    x_ref[pl.ds(1, side, 2), :] = result[:, half:]


def body(sol_map, resid_map, direction, precond, pixels, angle_index, angles, flag_mask, inv_noise, forms, twists):
    share_len = direction.shape[1]
    n_dev = lax.axis_size(DET_TM)
    n_pixels = share_len * n_dev
    map_rows = n_pixels // LANES
    share_rows = share_len // LANES
    det_rows, samples = pixels.shape
    total = det_rows * samples
    side = math.isqrt(total)
    f32 = jnp.float32

    pointing = jnp.stack([a.reshape(det_rows, samples // LANES, LANES) for a in (pixels, angle_index, flag_mask)], axis=1)
    pointing = exchange(pointing, TM)

    own = direction.reshape(1, 3 * share_rows, LANES)
    full = exchange(jnp.broadcast_to(own, (n_dev, 3 * share_rows, LANES)), DET_TM)

    trig = jnp.stack([jnp.cos(2.0 * angles), jnp.sin(2.0 * angles)])
    wide = (LANES, total // LANES)
    pix, weights, bounds, masks = pl.pallas_call(
        sort_kernel,
        in_specs=[VMEM, VMEM],
        out_specs=[VMEM] * 4,
        out_shape=[
            jax.ShapeDtypeStruct(wide, jnp.int32),
            jax.ShapeDtypeStruct((3, *wide), f32),
            jax.ShapeDtypeStruct((4, LANES), jnp.int32),
            jax.ShapeDtypeStruct((SLOTS, 8, LANES), jnp.int32),
        ],
        scratch_shapes=[pltpu.VMEM((total // LANES, LANES), jnp.int32)],
    )(pointing, trig)

    doubled = inv_noise[0, : total // 2].reshape(side // 2, side).T * 2.0
    corner = jnp.zeros((side, side // 2), jnp.bool_).at[0, 0].set(True)
    doubled = jnp.where(corner, inv_noise[0, 0], doubled)
    shares = pl.pallas_call(
        main_kernel,
        in_specs=[SMEM, SMEM] + [VMEM] * 7,
        out_specs=VMEM,
        out_shape=jax.ShapeDtypeStruct((2, n_dev // 2, 3 * share_rows, LANES), f32),
        scratch_shapes=[pltpu.VMEM((3, map_rows + 8, LANES), f32), pltpu.VMEM((total // LANES, LANES), f32), pltpu.VMEM(wide, f32)],
    )(bounds, inv_noise[0, total // 2 :], pix, weights, masks, full, forms, twists, doubled)

    shares = jnp.sum(exchange(shares, CORE), axis=0)
    image = jnp.sum(exchange(shares, CHIPS), axis=0).reshape(3, share_len)

    scaled_resid = precond * resid_map
    scalars = jnp.stack(
        [
            jnp.sum(scaled_resid * resid_map),
            jnp.sum(direction * image),
            jnp.sum(image * scaled_resid),
            jnp.sum(image * precond * image),
        ]
    )
    scalars = jnp.pad(scalars, (0, LANES - 4)).reshape(1, 1, LANES)
    scalars = jnp.sum(exchange(jnp.broadcast_to(scalars, (n_dev, 1, LANES)), DET_TM), axis=(0, 1))
    norm_old, curvature, cross_term, image_norm = scalars[0], scalars[1], scalars[2], scalars[3]
    step_size = norm_old / curvature
    new_resid = resid_map - step_size * image
    new_norm = norm_old - 2.0 * step_size * cross_term + step_size * step_size * image_norm
    new_sol = sol_map + step_size * direction
    new_dir = precond * new_resid + new_norm / norm_old * direction
    return (new_sol, new_resid, new_dir, new_norm)


def solution(mesh):
    split = Mesh(mesh.devices.reshape(mesh.shape["det"], 4, 4, 2), DET_TM)
    mapped = jax.shard_map(
        body,
        mesh=split,
        in_specs=(
            P(None, DET_TM),
            P(None, DET_TM),
            P(None, DET_TM),
            P(None, DET_TM),
            P("det", TM),
            P("det", TM),
            P(),
            P("det", TM),
            P(DET_TM, None),
            P(),
            P(),
        ),
        out_specs=(P(None, DET_TM), P(None, DET_TM), P(None, DET_TM), P()),
        check_vma=False,
    )

    def run(sol_map, resid_map, direction, precond, pixels, angle_index, angles, flag_mask, inv_noise):
        forms, twists = filter_tables(math.isqrt(pixels.shape[1]))
        return mapped(
            sol_map, resid_map, direction, precond, pixels, angle_index, angles, flag_mask, inv_noise, jnp.asarray(forms), jnp.asarray(twists)
        )

    return run
```

```python
import functools
import math

import jax
import jax.numpy as jnp
import numpy as np
from jax import lax
from jax.experimental import pallas as pl
from jax.experimental.pallas import tpu as pltpu
from jax.sharding import Mesh
from jax.sharding import PartitionSpec as P

DET_TM = ("det", "tm_0", "tm_1", "tm_2")
TM = ("tm_0", "tm_1", "tm_2")
CHIPS = ("det", "tm_0", "tm_1")
ROW = "det"
PLANE = ("tm_0", "tm_1")
CORE = "tm_2"

LANES = 128
CHUNK = 256
WINDOW = 16
ROWS = 16
VMEM = pl.BlockSpec(memory_space=pltpu.VMEM)
SMEM = pl.BlockSpec(memory_space=pltpu.SMEM)


def exchange(array, axes):
    return lax.all_to_all(array, axes, split_axis=0, concat_axis=0, tiled=True)


def halves(values):
    high = values.astype(jnp.bfloat16)
    return high, (values - high.astype(jnp.float32)).astype(jnp.bfloat16)


def dot(left, right, dims=(((1,), (0,)), ((), ()))):
    return lax.dot_general(left, right, dims, preferred_element_type=jnp.float32)


def dot3(left, right):
    return dot(left[0], right[0]) + (dot(left[0], right[1]) + dot(left[1], right[0]))


LEVELS = 16
CHUNK_BITS = 8
TILES = 64
SLOTS = LEVELS * (LEVELS - 1) + 2 * LEVELS


def tile(ref, index):
    return ref.at[8 * index : 8 * index + 8, :]


def sublane_step(bit):
    return 1 << (bit - 5 if bit < 8 else bit - 13)


def upper_half(bit):
    return lax.broadcasted_iota(jnp.int32, (8, LANES), 0) & sublane_step(bit)


def partner(values, bit):
    step = sublane_step(bit)
    if step == 4:
        return pltpu.roll(values, step, 0)
    return jnp.where(upper_half(bit) != 0, pltpu.roll(values, step, 0), pltpu.roll(values, 8 - step, 0))


def tile_pairs(bit):
    step = 1 << (bit if bit < 5 else 5 if bit == 8 else bit - 9)
    return [(i, i + step) for i in range(TILES) if not i & step]


def is_tile_bit(bit):
    return bit < 5 or 8 <= bit <= 12


def flip_blocks(ref):
    for part in range(ref.shape[0] // LANES):
        rows = slice(part * LANES, (part + 1) * LANES)
        ref[rows, :] = ref[rows, :].T


def word(position):
    return jnp.int32(-(1 << 31) if position == 31 else 1 << position)


def slot(level, bit):
    return level * (level - 1) + 2 * bit


def in_network(level, bit):
    return jnp.logical_and(bit < level, jnp.logical_or(level < LEVELS, bit >= CHUNK_BITS))


def place(tile_index):
    lane = lax.broadcasted_iota(jnp.int32, (8, LANES), 1)
    inside = lax.broadcasted_iota(jnp.int32, (8, LANES), 0) * 32 + ((lane & 7) << 13) + ((lane >> 3) << 9)
    return inside + ((tile_index & 31) + ((tile_index >> 5) << 8))


def sort_stage(key_ref, mask_ref, level, bit):
    at = slot(level, bit)
    if is_tile_bit(bit):
        bits = jnp.zeros((8, LANES), jnp.int32)
        for position, (low, high) in enumerate(tile_pairs(bit)):
            a, b = tile(key_ref, low)[...], tile(key_ref, high)[...]
            swap = a > b
            tile(key_ref, low)[...] = jnp.where(swap, b, a)
            tile(key_ref, high)[...] = jnp.where(swap, a, b)
            bits = bits | jnp.where(swap, word(position), 0)
        mask_ref[at] = bits
        return
    upper = jnp.where(upper_half(bit) != 0, -1, 0)
    for part in range(2):
        bits = jnp.zeros((8, LANES), jnp.int32)
        for position in range(32):
            view = tile(key_ref, 32 * part + position)
            own = view[...]
            other = partner(own, bit)
            swap = (own ^ upper) > (other ^ upper)
            view[...] = jnp.where(swap, other, own)
            bits = bits | jnp.where(swap, word(position), 0)
        mask_ref[at + part] = bits


def replay_stage(data_ref, mask_ref, level, bit):
    at = slot(level, bit)
    if is_tile_bit(bit):
        bits = mask_ref[at]
        for position, (low, high) in enumerate(tile_pairs(bit)):
            a, b = tile(data_ref, low)[...], tile(data_ref, high)[...]
            swap = (bits & word(position)) != 0
            tile(data_ref, low)[...] = jnp.where(swap, b, a)
            tile(data_ref, high)[...] = jnp.where(swap, a, b)
        return
    for part in range(2):
        bits = mask_ref[at + part]
        for position in range(32):
            view = tile(data_ref, 32 * part + position)
            own = view[...]
            view[...] = jnp.where((bits & word(position)) != 0, partner(own, bit), own)


def network(stage, ref, mask_ref, backwards=False, before=None):
    def one_level(count, carry):
        level = LEVELS - count if backwards else count + 1

        def run(bits):
            for bit in bits if backwards else reversed(bits):
                pl.when(in_network(level, bit))(functools.partial(stage, ref, mask_ref, level, bit))

        def flipped():
            flip_blocks(ref)
            run(range(9, LEVELS))
            flip_blocks(ref)

        if before is not None:
            before(level)
        if backwards:
            run(range(9))
        pl.when(level > 9)(flipped)
        if not backwards:
            run(range(9))
        return carry

    lax.fori_loop(0, LEVELS, one_level, 0)


def sort_kernel(pointing_ref, trig_ref, pix_ref, weight_ref, bound_ref, mask_ref, key_ref):
    blocks, _, block_rows, _ = pointing_ref.shape
    for block in range(blocks):
        packed = pointing_ref[block, 0] * 256 + pointing_ref[block, 1] * 2 + pointing_ref[block, 2]
        key_ref[block * block_rows : (block + 1) * block_rows, :] = packed
    for index in range(TILES):
        tile(key_ref, index)[...] ^= -(place(index) & 1)

    def turn(level):
        for index in range(TILES):
            at = place(index)
            tile(key_ref, index)[...] ^= -(((at >> level) ^ (at >> (level - 1))) & 1)

    network(sort_stage, key_ref, mask_ref, before=turn)

    half = key_ref.shape[0] // 2
    for h in range(2):
        keys = key_ref[h * half : (h + 1) * half, :]
        bound_ref[h : h + 1, :] = jnp.min(keys, axis=0, keepdims=True) >> 8
        bound_ref[2 + h : 3 + h, :] = jnp.max(keys, axis=0, keepdims=True) >> 8
    cos_row = jnp.broadcast_to(trig_ref[0:1, :], (8, LANES))
    sin_row = jnp.broadcast_to(trig_ref[1:2, :], (8, LANES))
    for part in range(4):
        keys = key_ref[part * LANES : (part + 1) * LANES, :].T
        cols = slice(part * LANES, (part + 1) * LANES)
        pix_ref[:, cols] = keys >> 8
        for row in range(0, LANES, 8):
            key = keys[row : row + 8]
            angle = (key >> 1) & (LANES - 1)
            usable = (key & 1).astype(jnp.float32)
            weight_ref[0, row : row + 8, cols] = usable
            weight_ref[1, row : row + 8, cols] = usable * jnp.take_along_axis(cos_row, angle, axis=1, mode="promise_in_bounds")
            weight_ref[2, row : row + 8, cols] = usable * jnp.take_along_axis(sin_row, angle, axis=1, mode="promise_in_bounds")


def one_hot_low(pixel_row):
    low = (pixel_row & (LANES - 1)).astype(jnp.float32).astype(jnp.bfloat16)
    level = lax.broadcasted_iota(jnp.int32, (LANES, CHUNK), 0).astype(jnp.float32).astype(jnp.bfloat16)
    return jnp.where(jnp.broadcast_to(low, level.shape) == level, jnp.bfloat16(1.0), jnp.bfloat16(0.0))


def window_mask(pixel_row, base):
    level = lax.broadcasted_iota(jnp.int32, (WINDOW, CHUNK), 0)
    return ((pixel_row >> 7) - base) == level


def gather_window(tab_ref, pixel_row, weight_rows, base):
    pieces = []
    for comp in range(3):
        pieces.extend(halves(tab_ref[comp, pl.ds(base, WINDOW), :]))
    found = dot(jnp.concatenate(pieces, axis=0), one_hot_low(pixel_row))
    total = None
    for comp in range(3):
        lo = 2 * comp * WINDOW
        value = (found[lo : lo + WINDOW] + found[lo + WINDOW : lo + 2 * WINDOW]) * weight_rows[comp]
        total = value if total is None else total + value
    return jnp.sum(jnp.where(window_mask(pixel_row, base), total, 0.0), axis=0, keepdims=True)


def first_base(bound_ref, row, half):
    return pl.multiple_of((bound_ref[half, row] >> 10) << 3, 8)


def window_count(bound_ref, row, half):
    return (((bound_ref[2 + half, row] >> 7) - first_base(bound_ref, row, half)) >> 4) + 1


def more_windows(bound_ref, head, one):
    counts = [window_count(bound_ref, head + r, h) for r in range(ROWS) for h in range(2)]

    @pl.when(functools.reduce(jnp.maximum, counts) > 1)
    def _():
        def each(r, carry):
            for h in range(2):
                base = first_base(bound_ref, head + r, h)

                def more(w, inner, h=h, base=base):
                    one(head + r, h, pl.multiple_of(base + w * WINDOW, 8))
                    return inner

                lax.fori_loop(1, window_count(bound_ref, head + r, h), more, 0)
            return carry

        lax.fori_loop(0, ROWS, each, 0)


def cut(values, r, h):
    return values[r : r + 1, h * CHUNK : (h + 1) * CHUNK]


def held(ref, row, h, *lead):
    return ref[(*lead, pl.ds(row, 1), slice(h * CHUNK, (h + 1) * CHUNK))]


def gather_all(bound_ref, pix_ref, weight_ref, tab_ref, out_ref):
    def step(it, carry):
        head = pl.multiple_of(it * ROWS, 8)
        pix = pix_ref[pl.ds(head, ROWS), :]
        weights = [weight_ref[comp, pl.ds(head, ROWS), :] for comp in range(3)]
        rows = []
        for r in range(ROWS):
            parts = [
                gather_window(tab_ref, cut(pix, r, h), [cut(w, r, h) for w in weights], first_base(bound_ref, head + r, h)) for h in range(2)
            ]
            rows.append(jnp.concatenate(parts, axis=1))
        out_ref[pl.ds(head, ROWS), :] = jnp.concatenate(rows, axis=0)

        def one(row, h, base):
            value = gather_window(tab_ref, held(pix_ref, row, h), [held(weight_ref, row, h, comp) for comp in range(3)], base)
            out_ref[pl.ds(row, 1), h * CHUNK : (h + 1) * CHUNK] += value

        more_windows(bound_ref, head, one)
        return carry

    lax.fori_loop(0, pix_ref.shape[0] // ROWS, step, 0)


def scatter_window(pixel_row, value_rows, base):
    mask = window_mask(pixel_row, base)
    pieces = []
    for value in value_rows:
        high = value.astype(jnp.bfloat16).astype(jnp.float32)
        for part in (high, value - high):
            pieces.append(jnp.where(mask, part, 0.0).astype(jnp.bfloat16))
    sums = dot(jnp.concatenate(pieces, axis=0), one_hot_low(pixel_row), (((1,), (1,)), ((), ())))
    return [sums[2 * c * WINDOW : (2 * c + 1) * WINDOW] + sums[(2 * c + 1) * WINDOW : (2 * c + 2) * WINDOW] for c in range(3)]


def scatter_all(bound_ref, pix_ref, weight_ref, value_ref, map_ref):
    map_ref[...] = jnp.zeros(map_ref.shape, jnp.float32)

    def add(sums, base):
        for comp in range(3):
            map_ref[comp, pl.ds(base, WINDOW), :] += sums[comp]

    def step(it, carry):
        head = pl.multiple_of(it * ROWS, 8)
        pix = pix_ref[pl.ds(head, ROWS), :]
        value = value_ref[pl.ds(head, ROWS), :]
        contrib = [value * weight_ref[comp, pl.ds(head, ROWS), :] for comp in range(3)]
        places = [(r, h) for r in range(ROWS) for h in range(2)]
        bases = [first_base(bound_ref, head + r, h) for r, h in places]
        sums = [scatter_window(cut(pix, r, h), [cut(c, r, h) for c in contrib], base) for (r, h), base in zip(places, bases)]
        for base, one_sum in zip(bases, sums):
            add(one_sum, base)

        def one(row, h, base):
            value = held(value_ref, row, h)
            add(scatter_window(held(pix_ref, row, h), [value * held(weight_ref, row, h, c) for c in range(3)], base), base)

        more_windows(bound_ref, head, one)
        return carry

    lax.fori_loop(0, pix_ref.shape[0] // ROWS, step, 0)


def main_kernel(
    bound_ref, tail_ref, here_ref, pix_ref, weight_ref, mask_ref, mine_ref, peer_ref, form_ref, twist_ref, filt_ref, keep_ref, send_ref, *scratch
):
    tab_ref, series_ref, wide_ref = scratch
    n_row = 4
    plane = mine_ref.shape[0]
    per_share = mine_ref.shape[1] // n_row
    share_rows = per_share // 3
    map_rows = plane * n_row * 2 * share_rows
    upper_core = here_ref[1] != 0

    def lay(spot, carry):
        for back in range(n_row):
            chip = ((here_ref[0] + (n_row - back)) & (n_row - 1)) * plane + spot
            row = pl.multiple_of(chip * 2 * share_rows, 8)
            for comp in range(3):
                piece = slice(back * per_share + comp * share_rows, back * per_share + (comp + 1) * share_rows)
                mine, peer = mine_ref[spot, piece, :], peer_ref[spot, piece, :]
                both = [jnp.where(upper_core, peer, mine), jnp.where(upper_core, mine, peer)]
                tab_ref[comp, pl.ds(row, 2 * share_rows), :] = jnp.concatenate(both, axis=0)
        return carry

    lax.fori_loop(0, plane, lay, 0)
    tab_ref[:, map_rows:, :] = jnp.zeros((3, tab_ref.shape[1] - map_rows, LANES), jnp.float32)

    gather_all(bound_ref, pix_ref, weight_ref, tab_ref, wide_ref)
    for part in range(4):
        series_ref[part * LANES : (part + 1) * LANES, :] = wide_ref[:, part * LANES : (part + 1) * LANES].T
    network(replay_stage, series_ref, mask_ref, backwards=True)
    filter_series(form_ref, twist_ref, filt_ref, tail_ref, series_ref)
    network(replay_stage, series_ref, mask_ref)
    for part in range(4):
        wide_ref[:, part * LANES : (part + 1) * LANES] = series_ref[part * LANES : (part + 1) * LANES, :].T
    scatter_all(bound_ref, pix_ref, weight_ref, wide_ref, tab_ref)

    def spread(couple, carry):
        row = pl.multiple_of(couple * 4 * share_rows, 8)
        sides = ([], [])
        for chip in range(2):
            for comp in range(3):
                both = tab_ref[comp, pl.ds(row + chip * 2 * share_rows, 2 * share_rows), :]
                low, high = both[:share_rows], both[share_rows:]
                sides[0].append(jnp.where(upper_core, high, low))
                sides[1].append(jnp.where(upper_core, low, high))
        at = pl.multiple_of(couple * 2 * per_share, 8)
        keep_ref[pl.ds(at, 2 * per_share), :] = jnp.concatenate(sides[0], axis=0)
        send_ref[pl.ds(at, 2 * per_share), :] = jnp.concatenate(sides[1], axis=0)
        return carry

    lax.fori_loop(0, plane * n_row // 2, spread, 0)


def filter_tables(side):
    index = np.arange(side)
    turn = 2.0 * np.pi / side * ((index[:, None] * index[None, :]) % side)
    twist = 2.0 * np.pi / (side * side) * (index[:, None] * index[None, :])

    def split(values):
        high = values.astype(np.float32).astype(jnp.bfloat16)
        return high, (values - high.astype(np.float64)).astype(np.float32).astype(jnp.bfloat16)

    forms = np.stack([*split(np.cos(turn)), *split(-np.sin(turn))])
    twists = np.stack([np.cos(twist), -np.sin(twist)]).astype(np.float32)
    return forms, twists


def filter_series(form_ref, twist_ref, weight_ref, tail_ref, x_ref):
    side = form_ref.shape[1]
    half = side // 2
    total = side * side
    f_real = (form_ref[0], form_ref[1])
    f_imag = (form_ref[2], form_ref[3])
    w_real, w_imag = twist_ref[0], twist_ref[1]
    x = jnp.concatenate([x_ref[pl.ds(0, side, 2), :], x_ref[pl.ds(1, side, 2), :]], axis=1)
    xs = halves(x)
    y_real = dot3(f_real, xs)
    y_imag = dot3(f_imag, xs)
    y_real, y_imag = halves(y_real * w_real - y_imag * w_imag), halves(y_real * w_imag + y_imag * w_real)
    left_real = (f_real[0][:, :half], f_real[1][:, :half])
    left_imag = (f_imag[0][:, :half], f_imag[1][:, :half])
    weight = weight_ref[...]
    z_real = halves((dot3(y_real, left_real) - dot3(y_imag, left_imag)) * weight)
    z_imag = halves((dot3(y_real, left_imag) + dot3(y_imag, left_real)) * weight)
    top_real = (f_real[0][:half], f_real[1][:half])
    top_imag = (f_imag[0][:half], f_imag[1][:half])
    v_real = dot3(z_real, top_real) + dot3(z_imag, top_imag)
    v_imag = dot3(z_imag, top_real) - dot3(z_real, top_imag)
    v_real, v_imag = halves(v_real * w_real + v_imag * w_imag), halves(v_imag * w_real - v_real * w_imag)
    result = dot3(f_real, v_real) + dot3(f_imag, v_imag)
    sign = jnp.where((lax.broadcasted_iota(jnp.int32, (1, side), 1) & 1) == 0, 1.0, -1.0)
    last = jnp.sum(jnp.sum(x, axis=0, keepdims=True) * sign, axis=1, keepdims=True) * tail_ref[0]
    result = (result + last * sign) * (1.0 / total)
    x_ref[pl.ds(0, side, 2), :] = result[:, :half]
    x_ref[pl.ds(1, side, 2), :] = result[:, half:]


def body(sol_map, resid_map, direction, precond, pixels, angle_index, angles, flag_mask, inv_noise, forms, twists):
    share_len = direction.shape[1]
    n_dev = lax.axis_size(DET_TM)
    n_pixels = share_len * n_dev
    map_rows = n_pixels // LANES
    share_rows = share_len // LANES
    det_rows, samples = pixels.shape
    total = det_rows * samples
    side = math.isqrt(total)
    f32 = jnp.float32

    pointing = jnp.stack([a.reshape(det_rows, samples // LANES, LANES) for a in (pixels, angle_index, flag_mask)], axis=1)
    pointing = exchange(pointing, TM)

    own = direction.reshape(3 * share_rows, LANES)
    n_row = lax.axis_size(ROW)
    parts = [own] + [lax.ppermute(own, ROW, [(j, (j + s) % n_row) for j in range(n_row)]) for s in range(1, n_row)]
    n_plane = lax.axis_size(PLANE)
    spread = jnp.broadcast_to(jnp.concatenate(parts)[None], (n_plane, n_row * 3 * share_rows, LANES))
    spread, pointing = lax.optimization_barrier((spread, pointing))
    mine = exchange(spread, PLANE)
    peer = lax.ppermute(mine, CORE, [(0, 1), (1, 0)])
    here = jnp.stack([lax.axis_index(ROW), lax.axis_index(CORE)]).astype(jnp.int32)

    trig = jnp.stack([jnp.cos(2.0 * angles), jnp.sin(2.0 * angles)])
    wide = (LANES, total // LANES)
    ordering = pl.pallas_call(
        sort_kernel,
        in_specs=[VMEM, VMEM],
        out_specs=[VMEM] * 4,
        out_shape=[
            jax.ShapeDtypeStruct(wide, jnp.int32),
            jax.ShapeDtypeStruct((3, *wide), f32),
            jax.ShapeDtypeStruct((4, LANES), jnp.int32),
            jax.ShapeDtypeStruct((SLOTS, 8, LANES), jnp.int32),
        ],
        scratch_shapes=[pltpu.VMEM((total // LANES, LANES), jnp.int32)],
    )
    pix, weights, bounds, masks = ordering(pointing, trig)

    doubled = inv_noise[0, : total // 2].reshape(side // 2, side).T * 2.0
    corner = jnp.zeros((side, side // 2), jnp.bool_).at[0, 0].set(True)
    doubled = jnp.where(corner, inv_noise[0, 0], doubled)
    halved = jax.ShapeDtypeStruct((n_dev // 2 * 3 * share_rows, LANES), f32)
    keep, send = pl.pallas_call(
        main_kernel,
        in_specs=[SMEM] * 3 + [VMEM] * 8,
        out_specs=[VMEM] * 2,
        out_shape=[halved] * 2,
        scratch_shapes=[pltpu.VMEM((3, map_rows + 8, LANES), f32), pltpu.VMEM((total // LANES, LANES), f32), pltpu.VMEM(wide, f32)],
    )(bounds, inv_noise[0, total // 2 :], here, pix, weights, masks, mine, peer, forms, twists, doubled)

    shares = (keep + lax.ppermute(send, CORE, [(0, 1), (1, 0)])).reshape(n_dev // 2, 3 * share_rows, LANES)
    image = jnp.sum(exchange(shares, CHIPS), axis=0).reshape(3, share_len)

    scaled_resid = precond * resid_map
    scalars = jnp.stack(
        [
            jnp.sum(scaled_resid * resid_map),
            jnp.sum(direction * image),
            jnp.sum(image * scaled_resid),
            jnp.sum(image * precond * image),
        ]
    )
    scalars = jnp.pad(scalars, (0, LANES - 4)).reshape(1, 1, LANES)
    scalars = jnp.sum(exchange(jnp.broadcast_to(scalars, (n_dev, 1, LANES)), DET_TM), axis=(0, 1))
    norm_old, curvature, cross_term, image_norm = scalars[0], scalars[1], scalars[2], scalars[3]
    step_size = norm_old / curvature
    new_resid = resid_map - step_size * image
    new_norm = norm_old - 2.0 * step_size * cross_term + step_size * step_size * image_norm
    new_sol = sol_map + step_size * direction
    new_dir = precond * new_resid + new_norm / norm_old * direction
    return (new_sol, new_resid, new_dir, new_norm)


def solution(mesh):
    split = Mesh(mesh.devices.reshape(mesh.shape["det"], 4, 4, 2), DET_TM)
    mapped = jax.shard_map(
        body,
        mesh=split,
        in_specs=(
            P(None, DET_TM),
            P(None, DET_TM),
            P(None, DET_TM),
            P(None, DET_TM),
            P("det", TM),
            P("det", TM),
            P(),
            P("det", TM),
            P(DET_TM, None),
            P(),
            P(),
        ),
        out_specs=(P(None, DET_TM), P(None, DET_TM), P(None, DET_TM), P()),
        check_vma=False,
    )

    def run(sol_map, resid_map, direction, precond, pixels, angle_index, angles, flag_mask, inv_noise):
        forms, twists = filter_tables(math.isqrt(pixels.shape[1]))
        return mapped(
            sol_map, resid_map, direction, precond, pixels, angle_index, angles, flag_mask, inv_noise, jnp.asarray(forms), jnp.asarray(twists)
        )

    return run
```

```python
import functools
import math

import jax
import jax.numpy as jnp
import numpy as np
from jax import lax
from jax.experimental import pallas as pl
from jax.experimental.pallas import tpu as pltpu
from jax.sharding import Mesh
from jax.sharding import PartitionSpec as P

DET_TM = ("det", "tm_0", "tm_1", "tm_2")
TM = ("tm_0", "tm_1", "tm_2")
CHIPS = ("det", "tm_0", "tm_1")
ROW = "det"
PLANE = ("tm_0", "tm_1")
CORE = "tm_2"

LANES = 128
CHUNK = 256
WINDOW = 16
ROWS = 16
VMEM = pl.BlockSpec(memory_space=pltpu.VMEM)
SMEM = pl.BlockSpec(memory_space=pltpu.SMEM)


def exchange(array, axes):
    return lax.all_to_all(array, axes, split_axis=0, concat_axis=0, tiled=True)


def halves(values):
    high = values.astype(jnp.bfloat16)
    return high, (values - high.astype(jnp.float32)).astype(jnp.bfloat16)


def dot(left, right, dims=(((1,), (0,)), ((), ()))):
    return lax.dot_general(left, right, dims, preferred_element_type=jnp.float32)


def dot3(left, right):
    return dot(left[0], right[0]) + (dot(left[0], right[1]) + dot(left[1], right[0]))


LEVELS = 16
CHUNK_BITS = 8
TILES = 64
SLOTS = LEVELS * (LEVELS - 1) + 2 * LEVELS


def tile(ref, index):
    return ref.at[8 * index : 8 * index + 8, :]


def sublane_step(bit):
    return 1 << (bit - 5 if bit < 8 else bit - 13)


def upper_half(bit):
    return lax.broadcasted_iota(jnp.int32, (8, LANES), 0) & sublane_step(bit)


def partner(values, bit):
    step = sublane_step(bit)
    if step == 4:
        return pltpu.roll(values, step, 0)
    return jnp.where(upper_half(bit) != 0, pltpu.roll(values, step, 0), pltpu.roll(values, 8 - step, 0))


def tile_pairs(bit):
    step = 1 << (bit if bit < 5 else 5 if bit == 8 else bit - 9)
    return [(i, i + step) for i in range(TILES) if not i & step]


def is_tile_bit(bit):
    return bit < 5 or 8 <= bit <= 12


def flip_blocks(ref):
    for part in range(ref.shape[0] // LANES):
        rows = slice(part * LANES, (part + 1) * LANES)
        ref[rows, :] = ref[rows, :].T


def word(position):
    return jnp.int32(-(1 << 31) if position == 31 else 1 << position)


def slot(level, bit):
    return level * (level - 1) + 2 * bit


def in_network(level, bit):
    return jnp.logical_and(bit < level, jnp.logical_or(level < LEVELS, bit >= CHUNK_BITS))


def place(tile_index):
    lane = lax.broadcasted_iota(jnp.int32, (8, LANES), 1)
    inside = lax.broadcasted_iota(jnp.int32, (8, LANES), 0) * 32 + ((lane & 7) << 13) + ((lane >> 3) << 9)
    return inside + ((tile_index & 31) + ((tile_index >> 5) << 8))


def sort_stage(key_ref, mask_ref, level, bit):
    at = slot(level, bit)
    if is_tile_bit(bit):
        bits = jnp.zeros((8, LANES), jnp.int32)
        for position, (low, high) in enumerate(tile_pairs(bit)):
            a, b = tile(key_ref, low)[...], tile(key_ref, high)[...]
            swap = a > b
            tile(key_ref, low)[...] = jnp.where(swap, b, a)
            tile(key_ref, high)[...] = jnp.where(swap, a, b)
            bits = bits | jnp.where(swap, word(position), 0)
        mask_ref[at] = bits
        return
    upper = jnp.where(upper_half(bit) != 0, -1, 0)
    for part in range(2):
        bits = jnp.zeros((8, LANES), jnp.int32)
        for position in range(32):
            view = tile(key_ref, 32 * part + position)
            own = view[...]
            other = partner(own, bit)
            swap = (own ^ upper) > (other ^ upper)
            view[...] = jnp.where(swap, other, own)
            bits = bits | jnp.where(swap, word(position), 0)
        mask_ref[at + part] = bits


def replay_stage(data_ref, mask_ref, level, bit):
    at = slot(level, bit)
    if is_tile_bit(bit):
        bits = mask_ref[at]
        for position, (low, high) in enumerate(tile_pairs(bit)):
            a, b = tile(data_ref, low)[...], tile(data_ref, high)[...]
            swap = (bits & word(position)) != 0
            tile(data_ref, low)[...] = jnp.where(swap, b, a)
            tile(data_ref, high)[...] = jnp.where(swap, a, b)
        return
    for part in range(2):
        bits = mask_ref[at + part]
        for position in range(32):
            view = tile(data_ref, 32 * part + position)
            own = view[...]
            view[...] = jnp.where((bits & word(position)) != 0, partner(own, bit), own)


def network(stage, ref, mask_ref, backwards=False, before=None):
    def one_level(count, carry):
        level = LEVELS - count if backwards else count + 1

        def run(bits):
            for bit in bits if backwards else reversed(bits):
                pl.when(in_network(level, bit))(functools.partial(stage, ref, mask_ref, level, bit))

        def flipped():
            flip_blocks(ref)
            run(range(9, LEVELS))
            flip_blocks(ref)

        if before is not None:
            before(level)
        if backwards:
            run(range(9))
        pl.when(level > 9)(flipped)
        if not backwards:
            run(range(9))
        return carry

    lax.fori_loop(0, LEVELS, one_level, 0)


def sort_kernel(pointing_ref, trig_ref, pix_ref, weight_ref, bound_ref, mask_ref, key_ref):
    blocks, _, block_rows, _ = pointing_ref.shape
    for block in range(blocks):
        packed = pointing_ref[block, 0] * 256 + pointing_ref[block, 1] * 2 + pointing_ref[block, 2]
        key_ref[block * block_rows : (block + 1) * block_rows, :] = packed
    for index in range(TILES):
        tile(key_ref, index)[...] ^= -(place(index) & 1)

    def turn(level):
        for index in range(TILES):
            at = place(index)
            tile(key_ref, index)[...] ^= -(((at >> level) ^ (at >> (level - 1))) & 1)

    network(sort_stage, key_ref, mask_ref, before=turn)

    half = key_ref.shape[0] // 2
    for h in range(2):
        keys = key_ref[h * half : (h + 1) * half, :]
        bound_ref[h : h + 1, :] = jnp.min(keys, axis=0, keepdims=True) >> 8
        bound_ref[2 + h : 3 + h, :] = jnp.max(keys, axis=0, keepdims=True) >> 8
    cos_row = jnp.broadcast_to(trig_ref[0:1, :], (8, LANES))
    sin_row = jnp.broadcast_to(trig_ref[1:2, :], (8, LANES))
    for part in range(4):
        keys = key_ref[part * LANES : (part + 1) * LANES, :].T
        cols = slice(part * LANES, (part + 1) * LANES)
        pix_ref[:, cols] = keys >> 8
        for row in range(0, LANES, 8):
            key = keys[row : row + 8]
            angle = (key >> 1) & (LANES - 1)
            usable = (key & 1).astype(jnp.float32)
            weight_ref[0, row : row + 8, cols] = usable
            weight_ref[1, row : row + 8, cols] = usable * jnp.take_along_axis(cos_row, angle, axis=1, mode="promise_in_bounds")
            weight_ref[2, row : row + 8, cols] = usable * jnp.take_along_axis(sin_row, angle, axis=1, mode="promise_in_bounds")


def one_hot_low(pixel_row):
    low = (pixel_row & (LANES - 1)).astype(jnp.float32).astype(jnp.bfloat16)
    level = lax.broadcasted_iota(jnp.int32, (LANES, CHUNK), 0).astype(jnp.float32).astype(jnp.bfloat16)
    return jnp.where(jnp.broadcast_to(low, level.shape) == level, jnp.bfloat16(1.0), jnp.bfloat16(0.0))


def window_mask(pixel_row, base):
    level = lax.broadcasted_iota(jnp.int32, (WINDOW, CHUNK), 0)
    return ((pixel_row >> 7) - base) == level


def gather_window(tab_ref, pixel_row, weight_rows, base):
    pieces = []
    for comp in range(3):
        pieces.extend(halves(tab_ref[comp, pl.ds(base, WINDOW), :]))
    found = dot(jnp.concatenate(pieces, axis=0), one_hot_low(pixel_row))
    total = None
    for comp in range(3):
        lo = 2 * comp * WINDOW
        value = (found[lo : lo + WINDOW] + found[lo + WINDOW : lo + 2 * WINDOW]) * weight_rows[comp]
        total = value if total is None else total + value
    return jnp.sum(jnp.where(window_mask(pixel_row, base), total, 0.0), axis=0, keepdims=True)


def first_base(bound_ref, row, half):
    return pl.multiple_of((bound_ref[half, row] >> 10) << 3, 8)


def window_count(bound_ref, row, half):
    return (((bound_ref[2 + half, row] >> 7) - first_base(bound_ref, row, half)) >> 4) + 1


def more_windows(bound_ref, head, one):
    counts = [window_count(bound_ref, head + r, h) for r in range(ROWS) for h in range(2)]

    @pl.when(functools.reduce(jnp.maximum, counts) > 1)
    def _():
        def each(r, carry):
            for h in range(2):
                base = first_base(bound_ref, head + r, h)

                def more(w, inner, h=h, base=base):
                    one(head + r, h, pl.multiple_of(base + w * WINDOW, 8))
                    return inner

                lax.fori_loop(1, window_count(bound_ref, head + r, h), more, 0)
            return carry

        lax.fori_loop(0, ROWS, each, 0)


def cut(values, r, h):
    return values[r : r + 1, h * CHUNK : (h + 1) * CHUNK]


def held(ref, row, h, *lead):
    return ref[(*lead, pl.ds(row, 1), slice(h * CHUNK, (h + 1) * CHUNK))]


def gather_all(bound_ref, pix_ref, weight_ref, tab_ref, out_ref):
    def step(it, carry):
        head = pl.multiple_of(it * ROWS, 8)
        pix = pix_ref[pl.ds(head, ROWS), :]
        weights = [weight_ref[comp, pl.ds(head, ROWS), :] for comp in range(3)]
        rows = []
        for r in range(ROWS):
            parts = [
                gather_window(tab_ref, cut(pix, r, h), [cut(w, r, h) for w in weights], first_base(bound_ref, head + r, h)) for h in range(2)
            ]
            rows.append(jnp.concatenate(parts, axis=1))
        out_ref[pl.ds(head, ROWS), :] = jnp.concatenate(rows, axis=0)

        def one(row, h, base):
            value = gather_window(tab_ref, held(pix_ref, row, h), [held(weight_ref, row, h, comp) for comp in range(3)], base)
            out_ref[pl.ds(row, 1), h * CHUNK : (h + 1) * CHUNK] += value

        more_windows(bound_ref, head, one)
        return carry

    lax.fori_loop(0, pix_ref.shape[0] // ROWS, step, 0)


def scatter_window(pixel_row, value_rows, base):
    mask = window_mask(pixel_row, base)
    pieces = []
    for value in value_rows:
        high = value.astype(jnp.bfloat16).astype(jnp.float32)
        for part in (high, value - high):
            pieces.append(jnp.where(mask, part, 0.0).astype(jnp.bfloat16))
    sums = dot(jnp.concatenate(pieces, axis=0), one_hot_low(pixel_row), (((1,), (1,)), ((), ())))
    return [sums[2 * c * WINDOW : (2 * c + 1) * WINDOW] + sums[(2 * c + 1) * WINDOW : (2 * c + 2) * WINDOW] for c in range(3)]


def scatter_all(bound_ref, pix_ref, weight_ref, value_ref, map_ref):
    map_ref[...] = jnp.zeros(map_ref.shape, jnp.float32)

    def add(sums, base):
        for comp in range(3):
            map_ref[comp, pl.ds(base, WINDOW), :] += sums[comp]

    def step(it, carry):
        head = pl.multiple_of(it * ROWS, 8)
        pix = pix_ref[pl.ds(head, ROWS), :]
        value = value_ref[pl.ds(head, ROWS), :]
        contrib = [value * weight_ref[comp, pl.ds(head, ROWS), :] for comp in range(3)]
        places = [(r, h) for r in range(ROWS) for h in range(2)]
        bases = [first_base(bound_ref, head + r, h) for r, h in places]
        sums = [scatter_window(cut(pix, r, h), [cut(c, r, h) for c in contrib], base) for (r, h), base in zip(places, bases)]
        for base, one_sum in zip(bases, sums):
            add(one_sum, base)

        def one(row, h, base):
            value = held(value_ref, row, h)
            add(scatter_window(held(pix_ref, row, h), [value * held(weight_ref, row, h, c) for c in range(3)], base), base)

        more_windows(bound_ref, head, one)
        return carry

    lax.fori_loop(0, pix_ref.shape[0] // ROWS, step, 0)


def main_kernel(
    bound_ref, tail_ref, here_ref, pix_ref, weight_ref, mask_ref, mine_ref, peer_ref, form_ref, twist_ref, filt_ref, keep_ref, send_ref, *scratch
):
    tab_ref, series_ref, wide_ref = scratch
    n_row = 4
    plane = mine_ref.shape[0]
    per_share = mine_ref.shape[1] // n_row
    share_rows = per_share // 3
    map_rows = plane * n_row * 2 * share_rows
    upper_core = here_ref[1] != 0

    def lay(spot, carry):
        for back in range(n_row):
            chip = ((here_ref[0] + (n_row - back)) & (n_row - 1)) * plane + spot
            row = pl.multiple_of(chip * 2 * share_rows, 8)
            for comp in range(3):
                piece = slice(back * per_share + comp * share_rows, back * per_share + (comp + 1) * share_rows)
                mine, peer = mine_ref[spot, piece, :], peer_ref[spot, piece, :]
                both = [jnp.where(upper_core, peer, mine), jnp.where(upper_core, mine, peer)]
                tab_ref[comp, pl.ds(row, 2 * share_rows), :] = jnp.concatenate(both, axis=0)
        return carry

    lax.fori_loop(0, plane, lay, 0)
    tab_ref[:, map_rows:, :] = jnp.zeros((3, tab_ref.shape[1] - map_rows, LANES), jnp.float32)

    gather_all(bound_ref, pix_ref, weight_ref, tab_ref, wide_ref)
    for part in range(4):
        series_ref[part * LANES : (part + 1) * LANES, :] = wide_ref[:, part * LANES : (part + 1) * LANES].T
    network(replay_stage, series_ref, mask_ref, backwards=True)
    filter_series(form_ref, twist_ref, filt_ref, tail_ref, series_ref)
    network(replay_stage, series_ref, mask_ref)
    for part in range(4):
        wide_ref[:, part * LANES : (part + 1) * LANES] = series_ref[part * LANES : (part + 1) * LANES, :].T
    scatter_all(bound_ref, pix_ref, weight_ref, wide_ref, tab_ref)

    def spread(couple, carry):
        row = pl.multiple_of(couple * 4 * share_rows, 8)
        sides = ([], [])
        for chip in range(2):
            for comp in range(3):
                both = tab_ref[comp, pl.ds(row + chip * 2 * share_rows, 2 * share_rows), :]
                low, high = both[:share_rows], both[share_rows:]
                sides[0].append(jnp.where(upper_core, high, low))
                sides[1].append(jnp.where(upper_core, low, high))
        at = pl.multiple_of(couple * 2 * per_share, 8)
        keep_ref[pl.ds(at, 2 * per_share), :] = jnp.concatenate(sides[0], axis=0)
        send_ref[pl.ds(at, 2 * per_share), :] = jnp.concatenate(sides[1], axis=0)
        return carry

    lax.fori_loop(0, plane * n_row // 2, spread, 0)


def filter_tables(side):
    index = np.arange(side)
    turn = 2.0 * np.pi / side * ((index[:, None] * index[None, :]) % side)
    twist = 2.0 * np.pi / (side * side) * (index[:, None] * index[None, :])

    def split(values):
        high = values.astype(np.float32).astype(jnp.bfloat16)
        return high, (values - high.astype(np.float64)).astype(np.float32).astype(jnp.bfloat16)

    forms = np.stack([*split(np.cos(turn)), *split(-np.sin(turn))])
    twists = np.stack([np.cos(twist), -np.sin(twist)]).astype(np.float32)
    return forms, twists


def filter_series(form_ref, twist_ref, weight_ref, tail_ref, x_ref):
    side = form_ref.shape[1]
    half = side // 2
    total = side * side
    f_real = (form_ref[0], form_ref[1])
    f_imag = (form_ref[2], form_ref[3])
    w_real, w_imag = twist_ref[0], twist_ref[1]
    x = jnp.concatenate([x_ref[pl.ds(0, side, 2), :], x_ref[pl.ds(1, side, 2), :]], axis=1)
    xs = halves(x)
    y_real = dot3(f_real, xs)
    y_imag = dot3(f_imag, xs)
    y_real, y_imag = halves(y_real * w_real - y_imag * w_imag), halves(y_real * w_imag + y_imag * w_real)
    left_real = (f_real[0][:, :half], f_real[1][:, :half])
    left_imag = (f_imag[0][:, :half], f_imag[1][:, :half])
    weight = weight_ref[...]
    z_real = halves((dot3(y_real, left_real) - dot3(y_imag, left_imag)) * weight)
    z_imag = halves((dot3(y_real, left_imag) + dot3(y_imag, left_real)) * weight)
    top_real = (f_real[0][:half], f_real[1][:half])
    top_imag = (f_imag[0][:half], f_imag[1][:half])
    v_real = dot3(z_real, top_real) + dot3(z_imag, top_imag)
    v_imag = dot3(z_imag, top_real) - dot3(z_real, top_imag)
    v_real, v_imag = halves(v_real * w_real + v_imag * w_imag), halves(v_imag * w_real - v_real * w_imag)
    result = dot3(f_real, v_real) + dot3(f_imag, v_imag)
    sign = jnp.where((lax.broadcasted_iota(jnp.int32, (1, side), 1) & 1) == 0, 1.0, -1.0)
    last = jnp.sum(jnp.sum(x, axis=0, keepdims=True) * sign, axis=1, keepdims=True) * tail_ref[0]
    result = (result + last * sign) * (1.0 / total)
    x_ref[pl.ds(0, side, 2), :] = result[:, :half]
    x_ref[pl.ds(1, side, 2), :] = result[:, half:]


def sums_kernel(shares_ref, resid_ref, direction_ref, precond_ref, image_ref, sums_ref):
    rows = jnp.sum(shares_ref[...], axis=0)
    share_rows = rows.shape[0] * rows.shape[1] // 3
    for comp in range(3):
        for j in range(share_rows):
            at = comp * share_rows + j
            image_ref[comp : comp + 1, j * LANES : (j + 1) * LANES] = rows[at // 4, at % 4 : at % 4 + 1]
    image = image_ref[...]
    scaled = precond_ref[...] * resid_ref[...]
    group = lax.broadcasted_iota(jnp.int32, (1, LANES), 1) >> 5
    merged = jnp.zeros((1, LANES), jnp.float32)
    for index, terms in enumerate((scaled * resid_ref[...], direction_ref[...] * image, image * scaled, image * precond_ref[...] * image)):
        row = jnp.sum(terms, axis=0, keepdims=True)
        row = functools.reduce(jnp.add, [row[:, j * LANES : (j + 1) * LANES] for j in range(share_rows)])
        row = row + pltpu.roll(row, 64, 1)
        row = row + pltpu.roll(row, 32, 1)
        merged = jnp.where(group == index, row, merged)
    sums_ref[...] = jnp.broadcast_to(merged.reshape(1, 1, LANES), sums_ref.shape)


def update_kernel(sums_ref, image_ref, sol_ref, resid_ref, direction_ref, precond_ref, new_sol_ref, new_resid_ref, new_dir_ref, norm_ref):
    row = jnp.sum(sums_ref[...], axis=0)
    group = lax.broadcasted_iota(jnp.int32, (1, LANES), 1) >> 5
    norm_old, curvature, cross_term, image_norm = (
        jnp.sum(jnp.where(group == index, row, 0.0), axis=1, keepdims=True) for index in range(4)
    )
    step_size = norm_old / curvature
    new_norm = norm_old - 2.0 * step_size * cross_term + step_size * step_size * image_norm
    direction = direction_ref[...]
    new_resid = resid_ref[...] - step_size * image_ref[...]
    new_resid_ref[...] = new_resid
    new_sol_ref[...] = sol_ref[...] + step_size * direction
    new_dir_ref[...] = precond_ref[...] * new_resid + (new_norm / norm_old) * direction
    norm_ref[...] = new_norm


def body(sol_map, resid_map, direction, precond, pixels, angle_index, angles, flag_mask, inv_noise, forms, twists):
    share_len = direction.shape[1]
    n_dev = lax.axis_size(DET_TM)
    n_pixels = share_len * n_dev
    map_rows = n_pixels // LANES
    share_rows = share_len // LANES
    det_rows, samples = pixels.shape
    total = det_rows * samples
    side = math.isqrt(total)
    f32 = jnp.float32

    pointing = jnp.stack([a.reshape(det_rows, samples // LANES, LANES) for a in (pixels, angle_index, flag_mask)], axis=1)
    pointing = exchange(pointing, TM)

    own = direction.reshape(3 * share_rows, LANES)
    n_row = lax.axis_size(ROW)
    parts = [own] + [lax.ppermute(own, ROW, [(j, (j + s) % n_row) for j in range(n_row)]) for s in range(1, n_row)]
    n_plane = lax.axis_size(PLANE)
    spread = jnp.broadcast_to(jnp.concatenate(parts)[None], (n_plane, n_row * 3 * share_rows, LANES))
    spread, pointing = lax.optimization_barrier((spread, pointing))
    mine = exchange(spread, PLANE)
    peer = lax.ppermute(mine, CORE, [(0, 1), (1, 0)])
    here = jnp.stack([lax.axis_index(ROW), lax.axis_index(CORE)]).astype(jnp.int32)

    trig = jnp.stack([jnp.cos(2.0 * angles), jnp.sin(2.0 * angles)])
    wide = (LANES, total // LANES)
    ordering = pl.pallas_call(
        sort_kernel,
        in_specs=[VMEM, VMEM],
        out_specs=[VMEM] * 4,
        out_shape=[
            jax.ShapeDtypeStruct(wide, jnp.int32),
            jax.ShapeDtypeStruct((3, *wide), f32),
            jax.ShapeDtypeStruct((4, LANES), jnp.int32),
            jax.ShapeDtypeStruct((SLOTS, 8, LANES), jnp.int32),
        ],
        scratch_shapes=[pltpu.VMEM((total // LANES, LANES), jnp.int32)],
    )
    pix, weights, bounds, masks = ordering(pointing, trig)

    doubled = inv_noise[0, : total // 2].reshape(side // 2, side).T * 2.0
    corner = jnp.zeros((side, side // 2), jnp.bool_).at[0, 0].set(True)
    doubled = jnp.where(corner, inv_noise[0, 0], doubled)
    halved = jax.ShapeDtypeStruct((n_dev // 2 * 3 * share_rows, LANES), f32)
    keep, send = pl.pallas_call(
        main_kernel,
        in_specs=[SMEM] * 3 + [VMEM] * 8,
        out_specs=[VMEM] * 2,
        out_shape=[halved] * 2,
        scratch_shapes=[pltpu.VMEM((3, map_rows + 8, LANES), f32), pltpu.VMEM((total // LANES, LANES), f32), pltpu.VMEM(wide, f32)],
    )(bounds, inv_noise[0, total // 2 :], here, pix, weights, masks, mine, peer, forms, twists, doubled)

    shares = (keep + lax.ppermute(send, CORE, [(0, 1), (1, 0)])).reshape(n_dev // 2, 3 * share_rows // 4, 4, LANES)
    own_map = jax.ShapeDtypeStruct((3, share_len), f32)
    image, sums = pl.pallas_call(
        sums_kernel, in_specs=[VMEM] * 4, out_specs=[VMEM] * 2, out_shape=[own_map, jax.ShapeDtypeStruct((n_dev, 1, LANES), f32)]
    )(exchange(shares, CHIPS), resid_map, direction, precond)
    new_sol, new_resid, new_dir, new_norm = pl.pallas_call(
        update_kernel, in_specs=[VMEM] * 6, out_specs=[VMEM] * 4, out_shape=[own_map] * 3 + [jax.ShapeDtypeStruct((1, 1), f32)]
    )(exchange(sums, DET_TM), image, sol_map, resid_map, direction, precond)
    return (new_sol, new_resid, new_dir, new_norm.reshape(()))


def solution(mesh):
    split = Mesh(mesh.devices.reshape(mesh.shape["det"], 4, 4, 2), DET_TM)
    mapped = jax.shard_map(
        body,
        mesh=split,
        in_specs=(
            P(None, DET_TM),
            P(None, DET_TM),
            P(None, DET_TM),
            P(None, DET_TM),
            P("det", TM),
            P("det", TM),
            P(),
            P("det", TM),
            P(DET_TM, None),
            P(),
            P(),
        ),
        out_specs=(P(None, DET_TM), P(None, DET_TM), P(None, DET_TM), P()),
        check_vma=False,
    )

    def run(sol_map, resid_map, direction, precond, pixels, angle_index, angles, flag_mask, inv_noise):
        forms, twists = filter_tables(math.isqrt(pixels.shape[1]))
        return mapped(
            sol_map, resid_map, direction, precond, pixels, angle_index, angles, flag_mask, inv_noise, jnp.asarray(forms), jnp.asarray(twists)
        )

    return run
```

```python
import functools
import math

import jax
import jax.numpy as jnp
import numpy as np
from jax import lax
from jax.experimental import pallas as pl
from jax.experimental.pallas import tpu as pltpu
from jax.sharding import Mesh
from jax.sharding import PartitionSpec as P

DET_TM = ("det", "tm_0", "tm_1", "tm_2")
TM = ("tm_0", "tm_1", "tm_2")
CHIPS = ("det", "tm_0", "tm_1")
ROW = "det"
PLANE = ("tm_0", "tm_1")
CORE = "tm_2"

LANES = 128
CHUNK = 256
WINDOW = 16
ROWS = 32
VMEM = pl.BlockSpec(memory_space=pltpu.VMEM)
SMEM = pl.BlockSpec(memory_space=pltpu.SMEM)


def exchange(array, axes):
    return lax.all_to_all(array, axes, split_axis=0, concat_axis=0, tiled=True)


def halves(values):
    high = values.astype(jnp.bfloat16)
    return high, (values - high.astype(jnp.float32)).astype(jnp.bfloat16)


def dot(left, right, dims=(((1,), (0,)), ((), ()))):
    return lax.dot_general(left, right, dims, preferred_element_type=jnp.float32)


def dot3(left, right):
    return dot(left[0], right[0]) + (dot(left[0], right[1]) + dot(left[1], right[0]))


LEVELS = 16
CHUNK_BITS = 8
TILES = 64
SLOTS = LEVELS * (LEVELS - 1) + 2 * LEVELS


def tile(ref, index):
    return ref.at[8 * index : 8 * index + 8, :]


def sublane_step(bit):
    return 1 << (bit - 5 if bit < 8 else bit - 13)


def upper_half(bit):
    return lax.broadcasted_iota(jnp.int32, (8, LANES), 0) & sublane_step(bit)


def partner(values, bit):
    step = sublane_step(bit)
    if step == 4:
        return pltpu.roll(values, step, 0)
    return jnp.where(upper_half(bit) != 0, pltpu.roll(values, step, 0), pltpu.roll(values, 8 - step, 0))


def tile_pairs(bit):
    step = 1 << (bit if bit < 5 else 5 if bit == 8 else bit - 9)
    return [(i, i + step) for i in range(TILES) if not i & step]


def is_tile_bit(bit):
    return bit < 5 or 8 <= bit <= 12


def flip_blocks(ref):
    for part in range(ref.shape[0] // LANES):
        rows = slice(part * LANES, (part + 1) * LANES)
        ref[rows, :] = ref[rows, :].T


def word(position):
    return jnp.int32(-(1 << 31) if position == 31 else 1 << position)


def slot(level, bit):
    return level * (level - 1) + 2 * bit


def in_network(level, bit):
    return jnp.logical_and(bit < level, jnp.logical_or(level < LEVELS, bit >= CHUNK_BITS))


def place(tile_index):
    lane = lax.broadcasted_iota(jnp.int32, (8, LANES), 1)
    inside = lax.broadcasted_iota(jnp.int32, (8, LANES), 0) * 32 + ((lane & 7) << 13) + ((lane >> 3) << 9)
    return inside + ((tile_index & 31) + ((tile_index >> 5) << 8))


def sort_stage(key_ref, mask_ref, level, bit):
    at = slot(level, bit)
    if is_tile_bit(bit):
        bits = jnp.zeros((8, LANES), jnp.int32)
        for position, (low, high) in enumerate(tile_pairs(bit)):
            a, b = tile(key_ref, low)[...], tile(key_ref, high)[...]
            swap = a > b
            tile(key_ref, low)[...] = jnp.where(swap, b, a)
            tile(key_ref, high)[...] = jnp.where(swap, a, b)
            bits = bits | jnp.where(swap, word(position), 0)
        mask_ref[at] = bits
        return
    upper = jnp.where(upper_half(bit) != 0, -1, 0)
    for part in range(2):
        bits = jnp.zeros((8, LANES), jnp.int32)
        for position in range(32):
            view = tile(key_ref, 32 * part + position)
            own = view[...]
            other = partner(own, bit)
            swap = (own ^ upper) > (other ^ upper)
            view[...] = jnp.where(swap, other, own)
            bits = bits | jnp.where(swap, word(position), 0)
        mask_ref[at + part] = bits


def replay_stage(data_ref, mask_ref, level, bit):
    at = slot(level, bit)
    if is_tile_bit(bit):
        bits = mask_ref[at]
        for position, (low, high) in enumerate(tile_pairs(bit)):
            a, b = tile(data_ref, low)[...], tile(data_ref, high)[...]
            swap = (bits & word(position)) != 0
            tile(data_ref, low)[...] = jnp.where(swap, b, a)
            tile(data_ref, high)[...] = jnp.where(swap, a, b)
        return
    for part in range(2):
        bits = mask_ref[at + part]
        for position in range(32):
            view = tile(data_ref, 32 * part + position)
            own = view[...]
            view[...] = jnp.where((bits & word(position)) != 0, partner(own, bit), own)


def network(stage, ref, mask_ref, backwards=False, before=None):
    def one_level(count, carry):
        level = LEVELS - count if backwards else count + 1

        def run(bits):
            for bit in bits if backwards else reversed(bits):
                pl.when(in_network(level, bit))(functools.partial(stage, ref, mask_ref, level, bit))

        def flipped():
            flip_blocks(ref)
            run(range(9, LEVELS))
            flip_blocks(ref)

        if before is not None:
            before(level)
        if backwards:
            run(range(9))
        pl.when(level > 9)(flipped)
        if not backwards:
            run(range(9))
        return carry

    lax.fori_loop(0, LEVELS, one_level, 0)


def sort_kernel(pointing_ref, trig_ref, pix_ref, weight_ref, bound_ref, mask_ref, key_ref):
    blocks, _, block_rows, _ = pointing_ref.shape
    for block in range(blocks):
        packed = pointing_ref[block, 0] * 256 + pointing_ref[block, 1] * 2 + pointing_ref[block, 2]
        key_ref[block * block_rows : (block + 1) * block_rows, :] = packed
    for index in range(TILES):
        tile(key_ref, index)[...] ^= -(place(index) & 1)

    def turn(level):
        for index in range(TILES):
            at = place(index)
            tile(key_ref, index)[...] ^= -(((at >> level) ^ (at >> (level - 1))) & 1)

    network(sort_stage, key_ref, mask_ref, before=turn)

    half = key_ref.shape[0] // 2
    for h in range(2):
        keys = key_ref[h * half : (h + 1) * half, :]
        bound_ref[h : h + 1, :] = jnp.min(keys, axis=0, keepdims=True) >> 8
        bound_ref[2 + h : 3 + h, :] = jnp.max(keys, axis=0, keepdims=True) >> 8
    cos_row = jnp.broadcast_to(trig_ref[0:1, :], (8, LANES))
    sin_row = jnp.broadcast_to(trig_ref[1:2, :], (8, LANES))
    for part in range(4):
        keys = key_ref[part * LANES : (part + 1) * LANES, :].T
        cols = slice(part * LANES, (part + 1) * LANES)
        pix_ref[:, cols] = keys >> 8
        for row in range(0, LANES, 8):
            key = keys[row : row + 8]
            angle = (key >> 1) & (LANES - 1)
            usable = (key & 1).astype(jnp.float32)
            weight_ref[0, row : row + 8, cols] = usable
            weight_ref[1, row : row + 8, cols] = usable * jnp.take_along_axis(cos_row, angle, axis=1, mode="promise_in_bounds")
            weight_ref[2, row : row + 8, cols] = usable * jnp.take_along_axis(sin_row, angle, axis=1, mode="promise_in_bounds")


def one_hot_low(pixel_row):
    low = (pixel_row & (LANES - 1)).astype(jnp.float32).astype(jnp.bfloat16)
    level = lax.broadcasted_iota(jnp.int32, (LANES, CHUNK), 0).astype(jnp.float32).astype(jnp.bfloat16)
    return jnp.where(jnp.broadcast_to(low, level.shape) == level, jnp.bfloat16(1.0), jnp.bfloat16(0.0))


def window_mask(pixel_row, base):
    level = lax.broadcasted_iota(jnp.int32, (WINDOW, CHUNK), 0)
    return ((pixel_row >> 7) - base) == level


def gather_window(tab_ref, pixel_row, weight_rows, base):
    pieces = []
    for comp in range(3):
        pieces.extend(halves(tab_ref[comp, pl.ds(base, WINDOW), :]))
    found = dot(jnp.concatenate(pieces, axis=0), one_hot_low(pixel_row))
    total = None
    for comp in range(3):
        lo = 2 * comp * WINDOW
        value = (found[lo : lo + WINDOW] + found[lo + WINDOW : lo + 2 * WINDOW]) * weight_rows[comp]
        total = value if total is None else total + value
    return jnp.sum(jnp.where(window_mask(pixel_row, base), total, 0.0), axis=0, keepdims=True)


def first_base(bound_ref, row, half):
    return pl.multiple_of((bound_ref[half, row] >> 10) << 3, 8)


def window_count(bound_ref, row, half):
    return (((bound_ref[2 + half, row] >> 7) - first_base(bound_ref, row, half)) >> 4) + 1


def more_windows(bound_ref, head, one):
    counts = [window_count(bound_ref, head + r, h) for r in range(ROWS) for h in range(2)]

    @pl.when(functools.reduce(jnp.maximum, counts) > 1)
    def _():
        def each(r, carry):
            for h in range(2):
                base = first_base(bound_ref, head + r, h)

                def more(w, inner, h=h, base=base):
                    one(head + r, h, pl.multiple_of(base + w * WINDOW, 8))
                    return inner

                lax.fori_loop(1, window_count(bound_ref, head + r, h), more, 0)
            return carry

        lax.fori_loop(0, ROWS, each, 0)


def cut(values, r, h):
    return values[r : r + 1, h * CHUNK : (h + 1) * CHUNK]


def held(ref, row, h, *lead):
    return ref[(*lead, pl.ds(row, 1), slice(h * CHUNK, (h + 1) * CHUNK))]


def gather_all(bound_ref, pix_ref, weight_ref, tab_ref, out_ref):
    def step(it, carry):
        head = pl.multiple_of(it * ROWS, 8)
        pix = pix_ref[pl.ds(head, ROWS), :]
        weights = [weight_ref[comp, pl.ds(head, ROWS), :] for comp in range(3)]
        rows = []
        for r in range(ROWS):
            parts = [
                gather_window(tab_ref, cut(pix, r, h), [cut(w, r, h) for w in weights], first_base(bound_ref, head + r, h)) for h in range(2)
            ]
            rows.append(jnp.concatenate(parts, axis=1))
        out_ref[pl.ds(head, ROWS), :] = jnp.concatenate(rows, axis=0)

        def one(row, h, base):
            value = gather_window(tab_ref, held(pix_ref, row, h), [held(weight_ref, row, h, comp) for comp in range(3)], base)
            out_ref[pl.ds(row, 1), h * CHUNK : (h + 1) * CHUNK] += value

        more_windows(bound_ref, head, one)
        return carry

    lax.fori_loop(0, pix_ref.shape[0] // ROWS, step, 0)


def scatter_window(pixel_row, value_rows, base):
    mask = window_mask(pixel_row, base)
    pieces = []
    for value in value_rows:
        high = value.astype(jnp.bfloat16).astype(jnp.float32)
        for part in (high, value - high):
            pieces.append(jnp.where(mask, part, 0.0).astype(jnp.bfloat16))
    sums = dot(jnp.concatenate(pieces, axis=0), one_hot_low(pixel_row), (((1,), (1,)), ((), ())))
    return [sums[2 * c * WINDOW : (2 * c + 1) * WINDOW] + sums[(2 * c + 1) * WINDOW : (2 * c + 2) * WINDOW] for c in range(3)]


def scatter_all(bound_ref, pix_ref, weight_ref, value_ref, map_ref):
    map_ref[...] = jnp.zeros(map_ref.shape, jnp.float32)

    def add(sums, base):
        for comp in range(3):
            map_ref[comp, pl.ds(base, WINDOW), :] += sums[comp]

    def step(it, carry):
        head = pl.multiple_of(it * ROWS, 8)
        pix = pix_ref[pl.ds(head, ROWS), :]
        value = value_ref[pl.ds(head, ROWS), :]
        contrib = [value * weight_ref[comp, pl.ds(head, ROWS), :] for comp in range(3)]
        places = [(r, h) for r in range(ROWS) for h in range(2)]
        bases = [first_base(bound_ref, head + r, h) for r, h in places]
        sums = [scatter_window(cut(pix, r, h), [cut(c, r, h) for c in contrib], base) for (r, h), base in zip(places, bases)]
        for base, one_sum in zip(bases, sums):
            add(one_sum, base)

        def one(row, h, base):
            value = held(value_ref, row, h)
            add(scatter_window(held(pix_ref, row, h), [value * held(weight_ref, row, h, c) for c in range(3)], base), base)

        more_windows(bound_ref, head, one)
        return carry

    lax.fori_loop(0, pix_ref.shape[0] // ROWS, step, 0)


def main_kernel(
    bound_ref, tail_ref, here_ref, pix_ref, weight_ref, mask_ref, mine_ref, peer_ref, form_ref, twist_ref, filt_ref, keep_ref, send_ref, *scratch
):
    tab_ref, series_ref, wide_ref = scratch
    n_row = 4
    plane = mine_ref.shape[0]
    per_share = mine_ref.shape[1] // n_row
    share_rows = per_share // 3
    map_rows = plane * n_row * 2 * share_rows
    upper_core = here_ref[1] != 0

    def lay(spot, carry):
        for back in range(n_row):
            chip = ((here_ref[0] + (n_row - back)) & (n_row - 1)) * plane + spot
            row = pl.multiple_of(chip * 2 * share_rows, 8)
            for comp in range(3):
                piece = slice(back * per_share + comp * share_rows, back * per_share + (comp + 1) * share_rows)
                mine, peer = mine_ref[spot, piece, :], peer_ref[spot, piece, :]
                both = [jnp.where(upper_core, peer, mine), jnp.where(upper_core, mine, peer)]
                tab_ref[comp, pl.ds(row, 2 * share_rows), :] = jnp.concatenate(both, axis=0)
        return carry

    lax.fori_loop(0, plane, lay, 0)
    tab_ref[:, map_rows:, :] = jnp.zeros((3, tab_ref.shape[1] - map_rows, LANES), jnp.float32)

    gather_all(bound_ref, pix_ref, weight_ref, tab_ref, wide_ref)
    for part in range(4):
        series_ref[part * LANES : (part + 1) * LANES, :] = wide_ref[:, part * LANES : (part + 1) * LANES].T
    network(replay_stage, series_ref, mask_ref, backwards=True)
    filter_series(form_ref, twist_ref, filt_ref, tail_ref, series_ref)
    network(replay_stage, series_ref, mask_ref)
    for part in range(4):
        wide_ref[:, part * LANES : (part + 1) * LANES] = series_ref[part * LANES : (part + 1) * LANES, :].T
    scatter_all(bound_ref, pix_ref, weight_ref, wide_ref, tab_ref)

    def spread(couple, carry):
        row = pl.multiple_of(couple * 4 * share_rows, 8)
        sides = ([], [])
        for chip in range(2):
            for comp in range(3):
                both = tab_ref[comp, pl.ds(row + chip * 2 * share_rows, 2 * share_rows), :]
                low, high = both[:share_rows], both[share_rows:]
                sides[0].append(jnp.where(upper_core, high, low))
                sides[1].append(jnp.where(upper_core, low, high))
        at = pl.multiple_of(couple * 2 * per_share, 8)
        keep_ref[pl.ds(at, 2 * per_share), :] = jnp.concatenate(sides[0], axis=0)
        send_ref[pl.ds(at, 2 * per_share), :] = jnp.concatenate(sides[1], axis=0)
        return carry

    lax.fori_loop(0, plane * n_row // 2, spread, 0)


def filter_tables(side):
    index = np.arange(side)
    turn = 2.0 * np.pi / side * ((index[:, None] * index[None, :]) % side)
    twist = 2.0 * np.pi / (side * side) * (index[:, None] * index[None, :])

    def split(values):
        high = values.astype(np.float32).astype(jnp.bfloat16)
        return high, (values - high.astype(np.float64)).astype(np.float32).astype(jnp.bfloat16)

    forms = np.stack([*split(np.cos(turn)), *split(-np.sin(turn))])
    twists = np.stack([np.cos(twist), -np.sin(twist)]).astype(np.float32)
    return forms, twists


def filter_series(form_ref, twist_ref, weight_ref, tail_ref, x_ref):
    side = form_ref.shape[1]
    half = side // 2
    total = side * side
    f_real = (form_ref[0], form_ref[1])
    f_imag = (form_ref[2], form_ref[3])
    w_real, w_imag = twist_ref[0], twist_ref[1]
    x = jnp.concatenate([x_ref[pl.ds(0, side, 2), :], x_ref[pl.ds(1, side, 2), :]], axis=1)
    xs = halves(x)
    y_real = dot3(f_real, xs)
    y_imag = dot3(f_imag, xs)
    y_real, y_imag = halves(y_real * w_real - y_imag * w_imag), halves(y_real * w_imag + y_imag * w_real)
    left_real = (f_real[0][:, :half], f_real[1][:, :half])
    left_imag = (f_imag[0][:, :half], f_imag[1][:, :half])
    weight = weight_ref[...]
    z_real = halves((dot3(y_real, left_real) - dot3(y_imag, left_imag)) * weight)
    z_imag = halves((dot3(y_real, left_imag) + dot3(y_imag, left_real)) * weight)
    top_real = (f_real[0][:half], f_real[1][:half])
    top_imag = (f_imag[0][:half], f_imag[1][:half])
    v_real = dot3(z_real, top_real) + dot3(z_imag, top_imag)
    v_imag = dot3(z_imag, top_real) - dot3(z_real, top_imag)
    v_real, v_imag = halves(v_real * w_real + v_imag * w_imag), halves(v_imag * w_real - v_real * w_imag)
    result = dot3(f_real, v_real) + dot3(f_imag, v_imag)
    sign = jnp.where((lax.broadcasted_iota(jnp.int32, (1, side), 1) & 1) == 0, 1.0, -1.0)
    last = jnp.sum(jnp.sum(x, axis=0, keepdims=True) * sign, axis=1, keepdims=True) * tail_ref[0]
    result = (result + last * sign) * (1.0 / total)
    x_ref[pl.ds(0, side, 2), :] = result[:, :half]
    x_ref[pl.ds(1, side, 2), :] = result[:, half:]


def message_kernel(pixels_ref, angle_ref, flag_ref, out_ref):
    det_rows, samples = pixels_ref.shape
    blocks = samples // LANES
    for which, ref in enumerate((pixels_ref, angle_ref, flag_ref)):
        for group in range(det_rows // 8):
            for block in range(blocks):
                at = group * 8 * 3 * blocks + which * blocks + block
                out_ref[pl.ds(at, 8, 3 * blocks), :] = ref[group * 8 : group * 8 + 8, block * LANES : (block + 1) * LANES]


def sums_kernel(shares_ref, resid_ref, direction_ref, precond_ref, image_ref, sums_ref):
    rows = jnp.sum(shares_ref[...], axis=0)
    share_rows = rows.shape[0] * rows.shape[1] // 3
    for comp in range(3):
        for j in range(share_rows):
            at = comp * share_rows + j
            image_ref[comp : comp + 1, j * LANES : (j + 1) * LANES] = rows[at // 4, at % 4 : at % 4 + 1]
    image = image_ref[...]
    scaled = precond_ref[...] * resid_ref[...]
    group = lax.broadcasted_iota(jnp.int32, (1, LANES), 1) >> 5
    merged = jnp.zeros((1, LANES), jnp.float32)
    for index, terms in enumerate((scaled * resid_ref[...], direction_ref[...] * image, image * scaled, image * precond_ref[...] * image)):
        row = jnp.sum(terms, axis=0, keepdims=True)
        row = functools.reduce(jnp.add, [row[:, j * LANES : (j + 1) * LANES] for j in range(share_rows)])
        row = row + pltpu.roll(row, 64, 1)
        row = row + pltpu.roll(row, 32, 1)
        merged = jnp.where(group == index, row, merged)
    sums_ref[...] = jnp.broadcast_to(merged.reshape(1, 1, LANES), sums_ref.shape)


def update_kernel(sums_ref, image_ref, sol_ref, resid_ref, direction_ref, precond_ref, new_sol_ref, new_resid_ref, new_dir_ref, norm_ref):
    row = jnp.sum(sums_ref[...], axis=0)
    group = lax.broadcasted_iota(jnp.int32, (1, LANES), 1) >> 5
    norm_old, curvature, cross_term, image_norm = (
        jnp.sum(jnp.where(group == index, row, 0.0), axis=1, keepdims=True) for index in range(4)
    )
    step_size = norm_old / curvature
    new_norm = norm_old - 2.0 * step_size * cross_term + step_size * step_size * image_norm
    direction = direction_ref[...]
    new_resid = resid_ref[...] - step_size * image_ref[...]
    new_resid_ref[...] = new_resid
    new_sol_ref[...] = sol_ref[...] + step_size * direction
    new_dir_ref[...] = precond_ref[...] * new_resid + (new_norm / norm_old) * direction
    norm_ref[...] = new_norm


def body(sol_map, resid_map, direction, precond, pixels, angle_index, angles, flag_mask, inv_noise, forms, twists):
    share_len = direction.shape[1]
    n_dev = lax.axis_size(DET_TM)
    n_pixels = share_len * n_dev
    map_rows = n_pixels // LANES
    share_rows = share_len // LANES
    det_rows, samples = pixels.shape
    total = det_rows * samples
    side = math.isqrt(total)
    f32 = jnp.float32

    blocks = samples // LANES
    pointing = pl.pallas_call(
        message_kernel, in_specs=[VMEM] * 3, out_specs=VMEM, out_shape=jax.ShapeDtypeStruct((det_rows * 3 * blocks, LANES), jnp.int32)
    )(pixels, angle_index, flag_mask).reshape(det_rows, 3, blocks, LANES)
    pointing = exchange(pointing, TM)

    own = direction.reshape(3 * share_rows, LANES)
    n_row = lax.axis_size(ROW)
    parts = [own] + [lax.ppermute(own, ROW, [(j, (j + s) % n_row) for j in range(n_row)]) for s in range(1, n_row)]
    n_plane = lax.axis_size(PLANE)
    column = jnp.concatenate(parts)[None]
    spread = jnp.broadcast_to(column, (n_plane, n_row * 3 * share_rows, LANES))
    spread, pointing = lax.optimization_barrier((spread, pointing))
    mine = exchange(spread, PLANE)
    peer = lax.ppermute(mine, CORE, [(0, 1), (1, 0)])
    here = jnp.stack([lax.axis_index(ROW), lax.axis_index(CORE)]).astype(jnp.int32)

    trig = jnp.stack([jnp.cos(2.0 * angles), jnp.sin(2.0 * angles)])
    wide = (LANES, total // LANES)
    ordering = pl.pallas_call(
        sort_kernel,
        in_specs=[VMEM, VMEM],
        out_specs=[VMEM] * 4,
        out_shape=[
            jax.ShapeDtypeStruct(wide, jnp.int32),
            jax.ShapeDtypeStruct((3, *wide), f32),
            jax.ShapeDtypeStruct((4, LANES), jnp.int32),
            jax.ShapeDtypeStruct((SLOTS, 8, LANES), jnp.int32),
        ],
        scratch_shapes=[pltpu.VMEM((total // LANES, LANES), jnp.int32)],
    )
    pix, weights, bounds, masks = ordering(pointing, trig)

    doubled = inv_noise[0, : total // 2].reshape(side // 2, side).T * 2.0
    corner = jnp.zeros((side, side // 2), jnp.bool_).at[0, 0].set(True)
    doubled = jnp.where(corner, inv_noise[0, 0], doubled)
    halved = jax.ShapeDtypeStruct((n_dev // 2 * 3 * share_rows, LANES), f32)
    keep, send = pl.pallas_call(
        main_kernel,
        in_specs=[SMEM] * 3 + [VMEM] * 8,
        out_specs=[VMEM] * 2,
        out_shape=[halved] * 2,
        scratch_shapes=[pltpu.VMEM((3, map_rows + 8, LANES), f32), pltpu.VMEM((total // LANES, LANES), f32), pltpu.VMEM(wide, f32)],
    )(bounds, inv_noise[0, total // 2 :], here, pix, weights, masks, mine, peer, forms, twists, doubled)

    shares = (keep + lax.ppermute(send, CORE, [(0, 1), (1, 0)])).reshape(n_dev // 2, 3 * share_rows // 4, 4, LANES)
    own_map = jax.ShapeDtypeStruct((3, share_len), f32)
    image, sums = pl.pallas_call(
        sums_kernel, in_specs=[VMEM] * 4, out_specs=[VMEM] * 2, out_shape=[own_map, jax.ShapeDtypeStruct((n_dev, 1, LANES), f32)]
    )(exchange(shares, CHIPS), resid_map, direction, precond)
    new_sol, new_resid, new_dir, new_norm = pl.pallas_call(
        update_kernel, in_specs=[VMEM] * 6, out_specs=[VMEM] * 4, out_shape=[own_map] * 3 + [jax.ShapeDtypeStruct((1, 1), f32)]
    )(exchange(sums, DET_TM), image, sol_map, resid_map, direction, precond)
    return (new_sol, new_resid, new_dir, new_norm.reshape(()))


def solution(mesh):
    split = Mesh(mesh.devices.reshape(mesh.shape["det"], 4, 4, 2), DET_TM)
    mapped = jax.shard_map(
        body,
        mesh=split,
        in_specs=(
            P(None, DET_TM),
            P(None, DET_TM),
            P(None, DET_TM),
            P(None, DET_TM),
            P("det", TM),
            P("det", TM),
            P(),
            P("det", TM),
            P(DET_TM, None),
            P(),
            P(),
        ),
        out_specs=(P(None, DET_TM), P(None, DET_TM), P(None, DET_TM), P()),
        check_vma=False,
    )

    def run(sol_map, resid_map, direction, precond, pixels, angle_index, angles, flag_mask, inv_noise):
        forms, twists = filter_tables(math.isqrt(pixels.shape[1]))
        return mapped(
            sol_map, resid_map, direction, precond, pixels, angle_index, angles, flag_mask, inv_noise, jnp.asarray(forms), jnp.asarray(twists)
        )

    return run
```

```python
import functools
import math

import jax
import jax.numpy as jnp
import numpy as np
from jax import lax
from jax.experimental import pallas as pl
from jax.experimental.pallas import tpu as pltpu
from jax.sharding import Mesh
from jax.sharding import PartitionSpec as P

DET_TM = ("det", "tm_0", "tm_1", "tm_2")
TM = ("tm_0", "tm_1", "tm_2")
CHIPS = ("det", "tm_0", "tm_1")
ROW = "det"
PLANE = ("tm_0", "tm_1")
CORE = "tm_2"

LANES = 128
CHUNK = 256
WINDOW = 16
ROWS = 32
VMEM = pl.BlockSpec(memory_space=pltpu.VMEM)
SMEM = pl.BlockSpec(memory_space=pltpu.SMEM)
LATE = pl.BlockSpec(memory_space=pl.ANY)


def exchange(array, axes):
    return lax.all_to_all(array, axes, split_axis=0, concat_axis=0, tiled=True)


def halves(values):
    high = values.astype(jnp.bfloat16)
    return high, (values - high.astype(jnp.float32)).astype(jnp.bfloat16)


def dot(left, right, dims=(((1,), (0,)), ((), ()))):
    return lax.dot_general(left, right, dims, preferred_element_type=jnp.float32)


def dot3(left, right):
    return dot(left[0], right[0]) + (dot(left[0], right[1]) + dot(left[1], right[0]))


LEVELS = 16
CHUNK_BITS = 8
TILES = 64
SLOTS = LEVELS * (LEVELS - 1) + 2 * LEVELS


def tile(ref, index):
    return ref.at[8 * index : 8 * index + 8, :]


def sublane_step(bit):
    return 1 << (bit - 5 if bit < 8 else bit - 13)


def upper_half(bit):
    return lax.broadcasted_iota(jnp.int32, (8, LANES), 0) & sublane_step(bit)


def partner(values, bit):
    step = sublane_step(bit)
    if step == 4:
        return pltpu.roll(values, step, 0)
    return jnp.where(upper_half(bit) != 0, pltpu.roll(values, step, 0), pltpu.roll(values, 8 - step, 0))


def tile_pairs(bit):
    step = 1 << (bit if bit < 5 else 5 if bit == 8 else bit - 9)
    return [(i, i + step) for i in range(TILES) if not i & step]


def is_tile_bit(bit):
    return bit < 5 or 8 <= bit <= 12


def flip_blocks(ref):
    for part in range(ref.shape[0] // LANES):
        rows = slice(part * LANES, (part + 1) * LANES)
        ref[rows, :] = ref[rows, :].T


def word(position):
    return jnp.int32(-(1 << 31) if position == 31 else 1 << position)


def slot(level, bit):
    return level * (level - 1) + 2 * bit


def in_network(level, bit):
    return jnp.logical_and(bit < level, jnp.logical_or(level < LEVELS, bit >= CHUNK_BITS))


def place(tile_index):
    lane = lax.broadcasted_iota(jnp.int32, (8, LANES), 1)
    inside = lax.broadcasted_iota(jnp.int32, (8, LANES), 0) * 32 + ((lane & 7) << 13) + ((lane >> 3) << 9)
    return inside + ((tile_index & 31) + ((tile_index >> 5) << 8))


def sort_stage(key_ref, mask_ref, level, bit):
    at = slot(level, bit)
    if is_tile_bit(bit):
        bits = jnp.zeros((8, LANES), jnp.int32)
        for position, (low, high) in enumerate(tile_pairs(bit)):
            a, b = tile(key_ref, low)[...], tile(key_ref, high)[...]
            swap = a > b
            tile(key_ref, low)[...] = jnp.where(swap, b, a)
            tile(key_ref, high)[...] = jnp.where(swap, a, b)
            bits = bits | jnp.where(swap, word(position), 0)
        mask_ref[at] = bits
        return
    upper = jnp.where(upper_half(bit) != 0, -1, 0)
    for part in range(2):
        bits = jnp.zeros((8, LANES), jnp.int32)
        for position in range(32):
            view = tile(key_ref, 32 * part + position)
            own = view[...]
            other = partner(own, bit)
            swap = (own ^ upper) > (other ^ upper)
            view[...] = jnp.where(swap, other, own)
            bits = bits | jnp.where(swap, word(position), 0)
        mask_ref[at + part] = bits


def replay_stage(data_ref, mask_ref, level, bit):
    at = slot(level, bit)
    if is_tile_bit(bit):
        bits = mask_ref[at]
        for position, (low, high) in enumerate(tile_pairs(bit)):
            a, b = tile(data_ref, low)[...], tile(data_ref, high)[...]
            swap = (bits & word(position)) != 0
            tile(data_ref, low)[...] = jnp.where(swap, b, a)
            tile(data_ref, high)[...] = jnp.where(swap, a, b)
        return
    for part in range(2):
        bits = mask_ref[at + part]
        for position in range(32):
            view = tile(data_ref, 32 * part + position)
            own = view[...]
            view[...] = jnp.where((bits & word(position)) != 0, partner(own, bit), own)


def network(stage, ref, mask_ref, backwards=False, before=None):
    def one_level(count, carry):
        level = LEVELS - count if backwards else count + 1

        def run(bits):
            for bit in bits if backwards else reversed(bits):
                pl.when(in_network(level, bit))(functools.partial(stage, ref, mask_ref, level, bit))

        def flipped():
            flip_blocks(ref)
            run(range(9, LEVELS))
            flip_blocks(ref)

        if before is not None:
            before(level)
        if backwards:
            run(range(9))
        pl.when(level > 9)(flipped)
        if not backwards:
            run(range(9))
        return carry

    lax.fori_loop(0, LEVELS, one_level, 0)


def sort_kernel(pointing_ref, trig_ref, pix_ref, weight_ref, bound_ref, mask_ref, key_ref):
    blocks, _, block_rows, _ = pointing_ref.shape
    for block in range(blocks):
        packed = pointing_ref[block, 0] * 256 + pointing_ref[block, 1] * 2 + pointing_ref[block, 2]
        key_ref[block * block_rows : (block + 1) * block_rows, :] = packed
    for index in range(TILES):
        tile(key_ref, index)[...] ^= -(place(index) & 1)

    def turn(level):
        for index in range(TILES):
            at = place(index)
            tile(key_ref, index)[...] ^= -(((at >> level) ^ (at >> (level - 1))) & 1)

    network(sort_stage, key_ref, mask_ref, before=turn)

    half = key_ref.shape[0] // 2
    for h in range(2):
        keys = key_ref[h * half : (h + 1) * half, :]
        bound_ref[h : h + 1, :] = jnp.min(keys, axis=0, keepdims=True) >> 8
        bound_ref[2 + h : 3 + h, :] = jnp.max(keys, axis=0, keepdims=True) >> 8
    cos_row = jnp.broadcast_to(trig_ref[0:1, :], (8, LANES))
    sin_row = jnp.broadcast_to(trig_ref[1:2, :], (8, LANES))
    for part in range(4):
        keys = key_ref[part * LANES : (part + 1) * LANES, :].T
        cols = slice(part * LANES, (part + 1) * LANES)
        pix_ref[:, cols] = keys >> 8
        for row in range(0, LANES, 8):
            key = keys[row : row + 8]
            angle = (key >> 1) & (LANES - 1)
            usable = (key & 1).astype(jnp.float32)
            weight_ref[0, row : row + 8, cols] = usable
            weight_ref[1, row : row + 8, cols] = usable * jnp.take_along_axis(cos_row, angle, axis=1, mode="promise_in_bounds")
            weight_ref[2, row : row + 8, cols] = usable * jnp.take_along_axis(sin_row, angle, axis=1, mode="promise_in_bounds")


def one_hot_low(pixel_row):
    low = (pixel_row & (LANES - 1)).astype(jnp.float32).astype(jnp.bfloat16)
    level = lax.broadcasted_iota(jnp.int32, (LANES, CHUNK), 0).astype(jnp.float32).astype(jnp.bfloat16)
    return jnp.where(jnp.broadcast_to(low, level.shape) == level, jnp.bfloat16(1.0), jnp.bfloat16(0.0))


def window_mask(pixel_row, base):
    level = lax.broadcasted_iota(jnp.int32, (WINDOW, CHUNK), 0)
    return ((pixel_row >> 7) - base) == level


def gather_window(tab_ref, pixel_row, weight_rows, base):
    pieces = []
    for comp in range(3):
        pieces.extend(halves(tab_ref[comp, pl.ds(base, WINDOW), :]))
    found = dot(jnp.concatenate(pieces, axis=0), one_hot_low(pixel_row))
    total = None
    for comp in range(3):
        lo = 2 * comp * WINDOW
        value = (found[lo : lo + WINDOW] + found[lo + WINDOW : lo + 2 * WINDOW]) * weight_rows[comp]
        total = value if total is None else total + value
    return jnp.sum(jnp.where(window_mask(pixel_row, base), total, 0.0), axis=0, keepdims=True)


def first_base(bound_ref, row, half):
    return pl.multiple_of((bound_ref[half, row] >> 10) << 3, 8)


def window_count(bound_ref, row, half):
    return (((bound_ref[2 + half, row] >> 7) - first_base(bound_ref, row, half)) >> 4) + 1


def more_windows(bound_ref, head, one):
    counts = [window_count(bound_ref, head + r, h) for r in range(ROWS) for h in range(2)]

    @pl.when(functools.reduce(jnp.maximum, counts) > 1)
    def _():
        def each(r, carry):
            for h in range(2):
                base = first_base(bound_ref, head + r, h)

                def more(w, inner, h=h, base=base):
                    one(head + r, h, pl.multiple_of(base + w * WINDOW, 8))
                    return inner

                lax.fori_loop(1, window_count(bound_ref, head + r, h), more, 0)
            return carry

        lax.fori_loop(0, ROWS, each, 0)


def cut(values, r, h):
    return values[r : r + 1, h * CHUNK : (h + 1) * CHUNK]


def held(ref, row, h, *lead):
    return ref[(*lead, pl.ds(row, 1), slice(h * CHUNK, (h + 1) * CHUNK))]


def gather_all(bound_ref, pix_ref, weight_ref, tab_ref, out_ref):
    def step(it, carry):
        head = pl.multiple_of(it * ROWS, 8)
        pix = pix_ref[pl.ds(head, ROWS), :]
        weights = [weight_ref[comp, pl.ds(head, ROWS), :] for comp in range(3)]
        rows = []
        for r in range(ROWS):
            parts = [
                gather_window(tab_ref, cut(pix, r, h), [cut(w, r, h) for w in weights], first_base(bound_ref, head + r, h)) for h in range(2)
            ]
            rows.append(jnp.concatenate(parts, axis=1))
        out_ref[pl.ds(head, ROWS), :] = jnp.concatenate(rows, axis=0)

        def one(row, h, base):
            value = gather_window(tab_ref, held(pix_ref, row, h), [held(weight_ref, row, h, comp) for comp in range(3)], base)
            out_ref[pl.ds(row, 1), h * CHUNK : (h + 1) * CHUNK] += value

        more_windows(bound_ref, head, one)
        return carry

    lax.fori_loop(0, pix_ref.shape[0] // ROWS, step, 0)


def scatter_window(pixel_row, value_rows, base):
    mask = window_mask(pixel_row, base)
    pieces = []
    for value in value_rows:
        high = value.astype(jnp.bfloat16).astype(jnp.float32)
        for part in (high, value - high):
            pieces.append(jnp.where(mask, part, 0.0).astype(jnp.bfloat16))
    sums = dot(jnp.concatenate(pieces, axis=0), one_hot_low(pixel_row), (((1,), (1,)), ((), ())))
    return [sums[2 * c * WINDOW : (2 * c + 1) * WINDOW] + sums[(2 * c + 1) * WINDOW : (2 * c + 2) * WINDOW] for c in range(3)]


def scatter_all(bound_ref, pix_ref, weight_ref, value_ref, map_ref):
    map_ref[...] = jnp.zeros(map_ref.shape, jnp.float32)

    def add(sums, base):
        for comp in range(3):
            map_ref[comp, pl.ds(base, WINDOW), :] += sums[comp]

    def step(it, carry):
        head = pl.multiple_of(it * ROWS, 8)
        pix = pix_ref[pl.ds(head, ROWS), :]
        value = value_ref[pl.ds(head, ROWS), :]
        contrib = [value * weight_ref[comp, pl.ds(head, ROWS), :] for comp in range(3)]
        places = [(r, h) for r in range(ROWS) for h in range(2)]
        bases = [first_base(bound_ref, head + r, h) for r, h in places]
        sums = [scatter_window(cut(pix, r, h), [cut(c, r, h) for c in contrib], base) for (r, h), base in zip(places, bases)]
        for base, one_sum in zip(bases, sums):
            add(one_sum, base)

        def one(row, h, base):
            value = held(value_ref, row, h)
            add(scatter_window(held(pix_ref, row, h), [value * held(weight_ref, row, h, c) for c in range(3)], base), base)

        more_windows(bound_ref, head, one)
        return carry

    lax.fori_loop(0, pix_ref.shape[0] // ROWS, step, 0)


def main_kernel(
    bound_ref, tail_ref, here_ref, pix_ref, weight_ref, mask_src, mine_ref, peer_ref, form_src, twist_src, filt_src, keep_ref, send_ref, *scratch
):
    tab_ref, series_ref, wide_ref, mask_ref, form_ref, twist_ref, filt_ref, arrived = scratch
    late = ((mask_src, mask_ref), (form_src, form_ref), (twist_src, twist_ref), (filt_src, filt_ref))
    late = [pltpu.make_async_copy(src, dst, arrived.at[i]) for i, (src, dst) in enumerate(late)]
    for copy in late:
        copy.start()
    n_row = 4
    plane = mine_ref.shape[0]
    per_share = mine_ref.shape[1] // n_row
    share_rows = per_share // 3
    map_rows = plane * n_row * 2 * share_rows
    upper_core = here_ref[1] != 0

    def lay(spot, carry):
        for back in range(n_row):
            chip = ((here_ref[0] + (n_row - back)) & (n_row - 1)) * plane + spot
            row = pl.multiple_of(chip * 2 * share_rows, 8)
            for comp in range(3):
                piece = slice(back * per_share + comp * share_rows, back * per_share + (comp + 1) * share_rows)
                mine, peer = mine_ref[spot, piece, :], peer_ref[spot, piece, :]
                both = [jnp.where(upper_core, peer, mine), jnp.where(upper_core, mine, peer)]
                tab_ref[comp, pl.ds(row, 2 * share_rows), :] = jnp.concatenate(both, axis=0)
        return carry

    lax.fori_loop(0, plane, lay, 0)
    tab_ref[:, map_rows:, :] = jnp.zeros((3, tab_ref.shape[1] - map_rows, LANES), jnp.float32)

    gather_all(bound_ref, pix_ref, weight_ref, tab_ref, wide_ref)
    for copy in late:
        copy.wait()
    for part in range(4):
        series_ref[part * LANES : (part + 1) * LANES, :] = wide_ref[:, part * LANES : (part + 1) * LANES].T
    network(replay_stage, series_ref, mask_ref, backwards=True)
    filter_series(form_ref, twist_ref, filt_ref, tail_ref, series_ref)
    network(replay_stage, series_ref, mask_ref)
    for part in range(4):
        wide_ref[:, part * LANES : (part + 1) * LANES] = series_ref[part * LANES : (part + 1) * LANES, :].T
    scatter_all(bound_ref, pix_ref, weight_ref, wide_ref, tab_ref)

    def spread(couple, carry):
        row = pl.multiple_of(couple * 4 * share_rows, 8)
        sides = ([], [])
        for chip in range(2):
            for comp in range(3):
                both = tab_ref[comp, pl.ds(row + chip * 2 * share_rows, 2 * share_rows), :]
                low, high = both[:share_rows], both[share_rows:]
                sides[0].append(jnp.where(upper_core, high, low))
                sides[1].append(jnp.where(upper_core, low, high))
        at = pl.multiple_of(couple * 2 * per_share, 8)
        keep_ref[pl.ds(at, 2 * per_share), :] = jnp.concatenate(sides[0], axis=0)
        send_ref[pl.ds(at, 2 * per_share), :] = jnp.concatenate(sides[1], axis=0)
        return carry

    lax.fori_loop(0, plane * n_row // 2, spread, 0)


def filter_tables(side):
    index = np.arange(side)
    turn = 2.0 * np.pi / side * ((index[:, None] * index[None, :]) % side)
    twist = 2.0 * np.pi / (side * side) * (index[:, None] * index[None, :])

    def split(values):
        high = values.astype(np.float32).astype(jnp.bfloat16)
        return high, (values - high.astype(np.float64)).astype(np.float32).astype(jnp.bfloat16)

    forms = np.stack([*split(np.cos(turn)), *split(-np.sin(turn))])
    twists = np.stack([np.cos(twist), -np.sin(twist)]).astype(np.float32)
    return forms, twists


def filter_series(form_ref, twist_ref, weight_ref, tail_ref, x_ref):
    side = form_ref.shape[1]
    half = side // 2
    total = side * side
    f_real = (form_ref[0], form_ref[1])
    f_imag = (form_ref[2], form_ref[3])
    w_real, w_imag = twist_ref[0], twist_ref[1]
    x = jnp.concatenate([x_ref[pl.ds(0, side, 2), :], x_ref[pl.ds(1, side, 2), :]], axis=1)
    xs = halves(x)
    y_real = dot3(f_real, xs)
    y_imag = dot3(f_imag, xs)
    y_real, y_imag = halves(y_real * w_real - y_imag * w_imag), halves(y_real * w_imag + y_imag * w_real)
    left_real = (f_real[0][:, :half], f_real[1][:, :half])
    left_imag = (f_imag[0][:, :half], f_imag[1][:, :half])
    weight = weight_ref[...]
    z_real = halves((dot3(y_real, left_real) - dot3(y_imag, left_imag)) * weight)
    z_imag = halves((dot3(y_real, left_imag) + dot3(y_imag, left_real)) * weight)
    top_real = (f_real[0][:half], f_real[1][:half])
    top_imag = (f_imag[0][:half], f_imag[1][:half])
    v_real = dot3(z_real, top_real) + dot3(z_imag, top_imag)
    v_imag = dot3(z_imag, top_real) - dot3(z_real, top_imag)
    v_real, v_imag = halves(v_real * w_real + v_imag * w_imag), halves(v_imag * w_real - v_real * w_imag)
    result = dot3(f_real, v_real) + dot3(f_imag, v_imag)
    sign = jnp.where((lax.broadcasted_iota(jnp.int32, (1, side), 1) & 1) == 0, 1.0, -1.0)
    last = jnp.sum(jnp.sum(x, axis=0, keepdims=True) * sign, axis=1, keepdims=True) * tail_ref[0]
    result = (result + last * sign) * (1.0 / total)
    x_ref[pl.ds(0, side, 2), :] = result[:, :half]
    x_ref[pl.ds(1, side, 2), :] = result[:, half:]


def message_kernel(pixels_ref, angle_ref, flag_ref, out_ref):
    det_rows, samples = pixels_ref.shape
    blocks = samples // LANES
    for which, ref in enumerate((pixels_ref, angle_ref, flag_ref)):
        for group in range(det_rows // 8):
            for block in range(blocks):
                at = group * 8 * 3 * blocks + which * blocks + block
                out_ref[pl.ds(at, 8, 3 * blocks), :] = ref[group * 8 : group * 8 + 8, block * LANES : (block + 1) * LANES]


def sums_kernel(shares_ref, resid_ref, direction_ref, precond_ref, image_ref, sums_ref):
    rows = jnp.sum(shares_ref[...], axis=0)
    share_rows = rows.shape[0] * rows.shape[1] // 3
    for comp in range(3):
        for j in range(share_rows):
            at = comp * share_rows + j
            image_ref[comp : comp + 1, j * LANES : (j + 1) * LANES] = rows[at // 4, at % 4 : at % 4 + 1]
    image = image_ref[...]
    scaled = precond_ref[...] * resid_ref[...]
    group = lax.broadcasted_iota(jnp.int32, (1, LANES), 1) >> 5
    merged = jnp.zeros((1, LANES), jnp.float32)
    for index, terms in enumerate((scaled * resid_ref[...], direction_ref[...] * image, image * scaled, image * precond_ref[...] * image)):
        row = jnp.sum(terms, axis=0, keepdims=True)
        row = functools.reduce(jnp.add, [row[:, j * LANES : (j + 1) * LANES] for j in range(share_rows)])
        row = row + pltpu.roll(row, 64, 1)
        row = row + pltpu.roll(row, 32, 1)
        merged = jnp.where(group == index, row, merged)
    sums_ref[...] = jnp.broadcast_to(merged.reshape(1, 1, LANES), sums_ref.shape)


def update_kernel(sums_ref, image_ref, sol_ref, resid_ref, direction_ref, precond_ref, new_sol_ref, new_resid_ref, new_dir_ref, norm_ref):
    row = jnp.sum(sums_ref[...], axis=0)
    group = lax.broadcasted_iota(jnp.int32, (1, LANES), 1) >> 5
    norm_old, curvature, cross_term, image_norm = (
        jnp.sum(jnp.where(group == index, row, 0.0), axis=1, keepdims=True) for index in range(4)
    )
    step_size = norm_old / curvature
    new_norm = norm_old - 2.0 * step_size * cross_term + step_size * step_size * image_norm
    direction = direction_ref[...]
    new_resid = resid_ref[...] - step_size * image_ref[...]
    new_resid_ref[...] = new_resid
    new_sol_ref[...] = sol_ref[...] + step_size * direction
    new_dir_ref[...] = precond_ref[...] * new_resid + (new_norm / norm_old) * direction
    norm_ref[...] = new_norm


def body(sol_map, resid_map, direction, precond, pixels, angle_index, angles, flag_mask, inv_noise, forms, twists):
    share_len = direction.shape[1]
    n_dev = lax.axis_size(DET_TM)
    n_pixels = share_len * n_dev
    map_rows = n_pixels // LANES
    share_rows = share_len // LANES
    det_rows, samples = pixels.shape
    total = det_rows * samples
    side = math.isqrt(total)
    f32 = jnp.float32

    blocks = samples // LANES
    pointing = pl.pallas_call(
        message_kernel, in_specs=[VMEM] * 3, out_specs=VMEM, out_shape=jax.ShapeDtypeStruct((det_rows * 3 * blocks, LANES), jnp.int32)
    )(pixels, angle_index, flag_mask).reshape(det_rows, 3, blocks, LANES)
    pointing = exchange(pointing, TM)

    own = direction.reshape(3 * share_rows, LANES)
    n_row = lax.axis_size(ROW)
    parts = [own] + [lax.ppermute(own, ROW, [(j, (j + s) % n_row) for j in range(n_row)]) for s in range(1, n_row)]
    n_plane = lax.axis_size(PLANE)
    column = jnp.concatenate(parts)[None]
    spread = jnp.broadcast_to(column, (n_plane, n_row * 3 * share_rows, LANES))
    spread, pointing = lax.optimization_barrier((spread, pointing))
    mine = exchange(spread, PLANE)
    peer = lax.ppermute(mine, CORE, [(0, 1), (1, 0)])
    here = jnp.stack([lax.axis_index(ROW), lax.axis_index(CORE)]).astype(jnp.int32)

    trig = jnp.stack([jnp.cos(2.0 * angles), jnp.sin(2.0 * angles)])
    wide = (LANES, total // LANES)
    ordering = pl.pallas_call(
        sort_kernel,
        in_specs=[VMEM, VMEM],
        out_specs=[VMEM] * 4,
        out_shape=[
            jax.ShapeDtypeStruct(wide, jnp.int32),
            jax.ShapeDtypeStruct((3, *wide), f32),
            jax.ShapeDtypeStruct((4, LANES), jnp.int32),
            jax.ShapeDtypeStruct((SLOTS, 8, LANES), jnp.int32),
        ],
        scratch_shapes=[pltpu.VMEM((total // LANES, LANES), jnp.int32)],
    )
    pix, weights, bounds, masks = ordering(pointing, trig)

    doubled = inv_noise[0, : total // 2].reshape(side // 2, side).T * 2.0
    corner = jnp.zeros((side, side // 2), jnp.bool_).at[0, 0].set(True)
    doubled = jnp.where(corner, inv_noise[0, 0], doubled)
    halved = jax.ShapeDtypeStruct((n_dev // 2 * 3 * share_rows, LANES), f32)
    keep, send = pl.pallas_call(
        main_kernel,
        in_specs=[SMEM] * 3 + [VMEM] * 2 + [LATE] + [VMEM] * 2 + [LATE] * 3,
        out_specs=[VMEM] * 2,
        out_shape=[halved] * 2,
        scratch_shapes=[
            pltpu.VMEM((3, map_rows + 8, LANES), f32),
            pltpu.VMEM((total // LANES, LANES), f32),
            pltpu.VMEM(wide, f32),
            *[pltpu.VMEM(a.shape, a.dtype) for a in (masks, forms, twists, doubled)],
            pltpu.SemaphoreType.DMA((4,)),
        ],
    )(bounds, inv_noise[0, total // 2 :], here, pix, weights, masks, mine, peer, forms, twists, doubled)

    shares = (keep + lax.ppermute(send, CORE, [(0, 1), (1, 0)])).reshape(n_dev // 2, 3 * share_rows // 4, 4, LANES)
    own_map = jax.ShapeDtypeStruct((3, share_len), f32)
    image, sums = pl.pallas_call(
        sums_kernel, in_specs=[VMEM] * 4, out_specs=[VMEM] * 2, out_shape=[own_map, jax.ShapeDtypeStruct((n_dev, 1, LANES), f32)]
    )(exchange(shares, CHIPS), resid_map, direction, precond)
    new_sol, new_resid, new_dir, new_norm = pl.pallas_call(
        update_kernel, in_specs=[VMEM] * 6, out_specs=[VMEM] * 4, out_shape=[own_map] * 3 + [jax.ShapeDtypeStruct((1, 1), f32)]
    )(exchange(sums, DET_TM), image, sol_map, resid_map, direction, precond)
    return (new_sol, new_resid, new_dir, new_norm.reshape(()))


def solution(mesh):
    split = Mesh(mesh.devices.reshape(mesh.shape["det"], 4, 4, 2), DET_TM)
    mapped = jax.shard_map(
        body,
        mesh=split,
        in_specs=(
            P(None, DET_TM),
            P(None, DET_TM),
            P(None, DET_TM),
            P(None, DET_TM),
            P("det", TM),
            P("det", TM),
            P(),
            P("det", TM),
            P(DET_TM, None),
            P(),
            P(),
        ),
        out_specs=(P(None, DET_TM), P(None, DET_TM), P(None, DET_TM), P()),
        check_vma=False,
    )

    def run(sol_map, resid_map, direction, precond, pixels, angle_index, angles, flag_mask, inv_noise):
        forms, twists = filter_tables(math.isqrt(pixels.shape[1]))
        return mapped(
            sol_map, resid_map, direction, precond, pixels, angle_index, angles, flag_mask, inv_noise, jnp.asarray(forms), jnp.asarray(twists)
        )

    return run
```
